8 devices in a mesh: rep: 1 (over z), fsdp: 2 (over y), ep: 4 (over x, core).
Axes of the slice: x: 2, y: 2, z: 1, core: 2. Of those that a mesh axis runs over, the one named last changes fastest.
Arguments:
- tokens: bfloat16 [4096, 1024], P(('rep', 'ep', 'fsdp'))
- expert_idx: int32 [4096, 8], P(('rep', 'ep', 'fsdp'))
- gates: float32 [4096, 8], P(('rep', 'ep', 'fsdp'))
- w_gate: bfloat16 [32, 1024, 512], P('ep', 'fsdp')
- w_up: bfloat16 [32, 1024, 512], P('ep', 'fsdp')
- w_down: bfloat16 [32, 512, 1024], P('ep', None, 'fsdp')
Outputs:
- output: bfloat16 [4096, 1024], P(('rep', 'ep', 'fsdp'))
All inputs are finite; a program needn't handle non-finite values.
Results may differ from the reference program's by a relative error of at most 0.001.
Values are sent between devices in bfloat16 or wider.
A program may use at most 1 GiB of HBM per device.

```python
import jax
import jax.numpy as jnp
from jax import lax

TOK_DEV = 512
MODEL_DIM = 1024
FFN_DIM = 512
NUM_EXPERTS = 32
TOP_K = 8
EP_SIZE = 4
FSDP_SIZE = 2

GROUP_DEVS = EP_SIZE * FSDP_SIZE
ROW_COUNT = GROUP_DEVS * TOK_DEV
CAPACITY = (2 * TOK_DEV * TOP_K + NUM_EXPERTS - 1) // NUM_EXPERTS


def route_draw(key):
    key_rank, key_noise = jax.random.split(key)
    ranks = jax.random.permutation(key_rank, NUM_EXPERTS)
    skew = (ranks * 768) // NUM_EXPERTS
    noise = jax.random.randint(key_noise, (ROW_COUNT, NUM_EXPERTS), 0, 1024)
    scores = (noise + skew[None, :]) * NUM_EXPERTS + jnp.arange(NUM_EXPERTS)[None, :]
    top_vals, chosen = lax.top_k(scores, TOP_K)
    return chosen.astype(jnp.int32)


def setup_inputs(seed: int = 0, part: int = 0) -> dict:
    part_key = jax.random.fold_in(jax.random.key(seed), part)
    key_tok, key_route, key_gate = jax.random.split(part_key, 3)
    key_wg, key_wu, key_wd = jax.random.split(jax.random.key(seed + 1), 3)
    tokens = jax.random.normal(key_tok, (ROW_COUNT, MODEL_DIM), jnp.float32).astype(jnp.bfloat16)
    expert_idx = route_draw(key_route)
    gates = jax.random.uniform(key_gate, (ROW_COUNT, TOP_K), jnp.float32, 0.2, 0.8)
    w_gate = (jax.random.normal(key_wg, (NUM_EXPERTS, MODEL_DIM, FFN_DIM), jnp.float32) * MODEL_DIM ** -0.5).astype(jnp.bfloat16)
    w_up = (jax.random.normal(key_wu, (NUM_EXPERTS, MODEL_DIM, FFN_DIM), jnp.float32) * MODEL_DIM ** -0.5).astype(jnp.bfloat16)
    w_down = (jax.random.normal(key_wd, (NUM_EXPERTS, FFN_DIM, MODEL_DIM), jnp.float32) * (2.0 * FFN_DIM ** -0.5)).astype(jnp.bfloat16)
    return {'tokens': tokens, 'expert_idx': expert_idx, 'gates': gates, 'w_gate': w_gate, 'w_up': w_up, 'w_down': w_down}


def block_slots(idx_block):
    flat_ids = idx_block.reshape(TOK_DEV * TOP_K)
    onehot = (flat_ids[:, None] == jnp.arange(NUM_EXPERTS)[None, :]).astype(jnp.int32)
    before = jnp.cumsum(onehot, axis=0) - onehot
    return jnp.sum(before * onehot, axis=1)


def reference(tokens, expert_idx, gates, w_gate, w_up, w_down):
    pair_count = ROW_COUNT * TOP_K
    slot_ids = lax.map(block_slots, expert_idx.reshape(GROUP_DEVS, TOK_DEV, TOP_K)).reshape(pair_count)
    flat_ids = expert_idx.reshape(pair_count)
    pair_pos = jnp.arange(pair_count)
    block_id = pair_pos // (TOK_DEV * TOP_K)
    tok_row = (pair_pos // TOP_K).astype(jnp.int32)
    per_expert = GROUP_DEVS * CAPACITY
    total_rows = NUM_EXPERTS * per_expert
    target = jnp.where(slot_ids < CAPACITY, flat_ids * per_expert + block_id * CAPACITY + slot_ids, total_rows)
    row_of = jnp.full((total_rows,), ROW_COUNT, jnp.int32).at[target].set(tok_row, mode='drop')
    gate_of = jnp.zeros((total_rows,), jnp.float32).at[target].set(gates.reshape(pair_count), mode='drop')
    padded = jnp.concatenate([tokens, jnp.zeros((1, MODEL_DIM), tokens.dtype)], axis=0)

    def expert_step(acc, stacked):
        wg_one, wu_one, wd_one, rows_one, gate_one = stacked
        picked = padded[rows_one]
        act_a = jnp.dot(picked, wg_one, preferred_element_type=jnp.float32)
        act_b = jnp.dot(picked, wu_one, preferred_element_type=jnp.float32)
        hidden = (jax.nn.silu(act_a) * act_b).astype(jnp.bfloat16)
        expert_out = jnp.dot(hidden, wd_one, preferred_element_type=jnp.float32).astype(jnp.bfloat16)
        acc = acc.at[rows_one].add(gate_one[:, None] * expert_out.astype(jnp.float32), mode='drop')
        return acc, None

    acc_init = jnp.zeros((ROW_COUNT, MODEL_DIM), jnp.float32)
    acc, unused = lax.scan(expert_step, acc_init, (w_gate, w_up, w_down, row_of.reshape(NUM_EXPERTS, per_expert), gate_of.reshape(NUM_EXPERTS, per_expert)))
    return (tokens.astype(jnp.float32) + acc).astype(jnp.bfloat16)
```

```python
import functools

import jax
import jax.numpy as jnp
from jax import lax
from jax.experimental import pallas as pl
from jax.experimental.pallas import tpu as pltpu
from jax.sharding import PartitionSpec as P

MESH = pl.DeviceIdType.MESH
OWN, XN, YN, DG = 0, 1, 2, 3


def moe_kernel(num_experts, capacity, chunk, tokens_hbm, idx_ref, gates_ref, wg_hbm, wu_hbm, wd_hbm, out_ref,
               tok, w, acc, hid, gt_send, gt_recv, gcol, rx, ry,
               loc_tok_sem, tok_send, tok_recv, g_send, g_recv_sem, loc_sem, ys_sem, yr_sem,
               po_s, po_r, pf_s, pf_r, cx_s, cx_r, cy_s, cy_r):
    rows, width = out_ref.shape
    n_local = wg_hbm.shape[0]
    n_own = n_local // 2
    half_w = width // 2
    half = rows // 2
    n_chunk = half // chunk
    ep = lax.axis_index("ep")
    y = lax.axis_index("fsdp")
    c = lax.rem(ep, 2)
    x = ep // 2
    oy = 1 - y
    x_dev = {"ep": lax.rem(ep + 2, 4), "fsdp": y}
    y_dev = {"ep": ep, "fsdp": oy}
    d_dev = {"ep": lax.rem(ep + 2, 4), "fsdp": oy}
    p_dev = {"ep": ep + 1 - 2 * c, "fsdp": y}
    w_hbm = (wg_hbm, wu_hbm, wd_hbm)

    def remote(src, dst, s, r, dev):
        return pltpu.make_async_remote_copy(src_ref=src, dst_ref=dst, send_sem=s, recv_sem=r, device_id=dev, device_id_type=MESH)

    def block(b):
        return tok.at[pl.ds(b * rows, rows)]

    barrier = pltpu.get_barrier_semaphore()
    for dev in (x_dev, y_dev, d_dev, p_dev):
        pl.semaphore_signal(barrier, inc=1, device_id=dev, device_id_type=MESH)
    pl.semaphore_wait(barrier, 4)

    tok_y = remote(tokens_hbm, block(YN), tok_send.at[0], tok_recv.at[0], y_dev)
    tok_x = remote(tokens_hbm, block(XN), tok_send.at[1], tok_recv.at[1], x_dev)
    tok_d = remote(block(YN), block(DG), tok_send.at[2], tok_recv.at[2], x_dev)
    tok_l = pltpu.make_async_copy(tokens_hbm, block(OWN), loc_tok_sem)
    tok_y.start()
    tok_x.start()
    tok_l.start()

    lane = lax.broadcasted_iota(jnp.int32, (1, 128), 1)
    dest, slot = lane // n_local, lax.rem(lane, n_local)
    dx, dy = lax.rem(dest, 2), dest // 2
    ex = x + dx - 2 * x * dx
    ey = y + dy - 2 * y * dy
    sc = slot // n_own
    ec = c + sc - 2 * c * sc
    expert = (2 * ex + ec) * n_local + ey * n_own + lax.rem(slot, n_own)
    expert = jnp.where(lane < num_experts, expert, -1)
    dense = jnp.zeros((rows, 128), jnp.float32)
    chosen = jnp.zeros((rows, 128), jnp.float32)
    for j in range(idx_ref.shape[1]):
        hit = idx_ref[:, j:j + 1] == expert
        dense = jnp.where(hit, gates_ref[:, j:j + 1], dense)
        chosen = jnp.where(hit, 1.0, chosen)
    before = lax.broadcasted_iota(jnp.int32, (rows, rows), 1) < lax.broadcasted_iota(jnp.int32, (rows, rows), 0)
    taken = jnp.dot(before.astype(jnp.bfloat16), chosen.astype(jnp.bfloat16), preferred_element_type=jnp.float32)
    dense = jnp.where(taken < float(capacity), dense, 0.0)
    gt_send[...] = dense.T
    g_copies = []
    for k, (b, dev) in enumerate(((XN, x_dev), (YN, y_dev), (DG, d_dev))):
        cp = remote(gt_send.at[pl.ds(b * n_local, n_local)], gt_recv.at[k], g_send.at[k], g_recv_sem.at[k], dev)
        cp.start()
        g_copies.append(cp)
    gcol[0] = dense

    def local_w(m, i):
        return pltpu.make_async_copy(w_hbm[m].at[y * n_own + i], w.at[m, i, y], loc_sem.at[m, i])

    def send_w(m, i):
        return remote(w_hbm[m].at[oy * n_own + i], w.at[m, i, y], ys_sem.at[m, i], yr_sem.at[m, i], y_dev)

    def arrived_w(m, i):
        return remote(w_hbm[m].at[oy * n_own + i], w.at[m, i, oy], ys_sem.at[m, i], yr_sem.at[m, i], y_dev)

    def partner_own(m, i):
        return remote(w_hbm[m].at[y * n_own + i], w.at[m, n_own + i, y], po_s.at[m, i], po_r.at[m, i], p_dev)

    def partner_fwd(m, i):
        return remote(w.at[m, i, oy], w.at[m, n_own + i, oy], pf_s.at[m, i], pf_r.at[m, i], p_dev)

    for i in range(n_own):
        for m in range(3):
            send_w(m, i).start()
    for i in range(n_own):
        for m in range(3):
            local_w(m, i).start()
            partner_own(m, i).start()

    tok_y.wait_recv()
    tok_d.start()
    for k, b in enumerate((XN, YN, DG)):
        g_copies[k].wait_recv()
        padded = jnp.concatenate([gt_recv[k], jnp.zeros((128 - n_local, rows), jnp.float32)], axis=0)
        gcol[b] = padded.T

    tok_l.wait()
    tok_x.wait_recv()
    tok_d.wait_recv()

    lane2 = lax.broadcasted_iota(jnp.int32, (1, 128), 1)

    def gate_up(k, s):
        wg = w[0, s].reshape(width, w.shape[-1])
        wu = w[1, s].reshape(width, w.shape[-1])

        def step(b, carry):
            at = pl.ds(pl.multiple_of(b * rows, rows), rows)
            r = tok[at, :]
            a = jnp.dot(r, wg, preferred_element_type=jnp.float32)
            u = jnp.dot(r, wu, preferred_element_type=jnp.float32)
            hid[k, at, :] = (a * jax.nn.sigmoid(a) * u).astype(jnp.bfloat16)
            return carry

        lax.fori_loop(0, 4, step, 0)

    def weighted(k, s, b, row, n, part):
        at = pl.ds(pl.multiple_of(b * rows + row, chunk), n)
        g = jnp.sum(jnp.where(lane2 == s, gcol[b, pl.ds(pl.multiple_of(row, chunk), n), :], 0.0), axis=1, keepdims=True)
        o = jnp.dot(hid[k, at, :], w[2, s, part], preferred_element_type=jnp.float32).astype(jnp.bfloat16).astype(jnp.float32)
        return jnp.where(g != 0.0, g * o, 0.0)

    def down(k, s, first):
        def step(b, carry):
            at = pl.ds(pl.multiple_of(b * rows, rows), rows)
            for part in range(2):
                cols = pl.ds(part * half_w, half_w)
                term = weighted(k, s, b, 0, rows, part)
                acc[at, cols] = jnp.where(first, 0.0, acc[at, cols]) + term
            return carry

        lax.fori_loop(0, 4, step, 0)

    def arrive(m, i):
        arrived_w(m, i).wait_recv()
        partner_fwd(m, i).start()

    def from_partner(m, i):
        partner_own(m, i).wait_recv()
        partner_fwd(m, i).wait_recv()

    def first_half(i):
        for m in range(2):
            arrive(m, i)
            local_w(m, i).wait()
        gate_up(0, i)
        for m in range(2):
            from_partner(m, i)
        gate_up(1, n_own + i)
        arrive(2, i)
        local_w(2, i).wait()

    def round_step(i, carry):
        first_half(i)
        down(0, i, i == 0)
        from_partner(2, i)
        down(1, n_own + i, False)
        return carry

    lax.fori_loop(0, n_own - 1, round_step, 0)
    last = n_own - 1
    first_half(last)
    from_partner(2, last)

    def finish(b, row, n):
        at = pl.ds(pl.multiple_of(b * rows + row, chunk), n)
        for part in range(2):
            cols = pl.ds(part * half_w, half_w)
            acc[at, cols] = (acc[at, cols] + weighted(0, last, b, row, n, part)) + weighted(1, n_own + last, b, row, n, part)

    def part_of(b, row):
        return acc.at[pl.ds(pl.multiple_of(b * rows + row, chunk), chunk)]

    def send_x(kind, k):
        b, base = ((DG, 0), (XN, 0), (XN, half))[kind]
        return remote(part_of(b, base + k * chunk), rx.at[kind, pl.ds(pl.multiple_of(k * chunk, chunk), chunk)],
                      cx_s.at[kind, k], cx_r.at[kind, k], x_dev)

    def send_y(kind, k):
        b, base = ((DG, half), (YN, half), (YN, 0))[kind]
        return remote(part_of(b, base + k * chunk), ry.at[kind, pl.ds(pl.multiple_of(k * chunk, chunk), chunk)],
                      cy_s.at[kind, k], cy_r.at[kind, k], y_dev)

    def diag_step(k, carry):
        finish(DG, k * chunk, chunk)
        send_x(0, k).start()
        finish(DG, half + k * chunk, chunk)
        send_y(0, k).start()
        return carry

    lax.fori_loop(0, n_chunk, diag_step, 0)

    def direct_step(k, carry):
        finish(XN, k * chunk, chunk)
        send_x(1, k).start()
        finish(YN, half + k * chunk, chunk)
        send_y(1, k).start()
        return carry

    lax.fori_loop(0, n_chunk, direct_step, 0)

    def passed_step(k, carry):
        at_x = pl.ds(pl.multiple_of(XN * rows + half + k * chunk, chunk), chunk)
        at_y = pl.ds(pl.multiple_of(YN * rows + k * chunk, chunk), chunk)
        here = pl.ds(pl.multiple_of(k * chunk, chunk), chunk)
        finish(YN, k * chunk, chunk)
        finish(XN, half + k * chunk, chunk)
        send_x(0, k).wait_recv()
        acc[at_y, :] = acc[at_y, :] + rx[0, here, :]
        send_y(2, k).start()
        send_y(0, k).wait_recv()
        acc[at_x, :] = acc[at_x, :] + ry[0, here, :]
        send_x(2, k).start()
        return carry

    lax.fori_loop(0, n_chunk, passed_step, 0)
    finish(OWN, 0, rows)

    def direct_add(k, carry):
        here = pl.ds(pl.multiple_of(k * chunk, chunk), chunk)
        there = pl.ds(pl.multiple_of(half + k * chunk, chunk), chunk)
        send_x(1, k).wait_recv()
        acc[here, :] = acc[here, :] + rx[1, here, :]
        send_y(1, k).wait_recv()
        acc[there, :] = acc[there, :] + ry[1, here, :]
        return carry

    lax.fori_loop(0, n_chunk, direct_add, 0)

    def last_add(k, carry):
        here = pl.ds(pl.multiple_of(k * chunk, chunk), chunk)
        there = pl.ds(pl.multiple_of(half + k * chunk, chunk), chunk)
        send_y(2, k).wait_recv()
        out_ref[here, :] = (tok[here, :].astype(jnp.float32) + (acc[here, :] + ry[2, here, :])).astype(out_ref.dtype)
        send_x(2, k).wait_recv()
        out_ref[there, :] = (tok[there, :].astype(jnp.float32) + (acc[there, :] + rx[2, here, :])).astype(out_ref.dtype)
        return carry

    lax.fori_loop(0, n_chunk, last_add, 0)

    def drain_w(i, carry):
        for m in range(3):
            send_w(m, i).wait_send()
            partner_own(m, i).wait_send()
            partner_fwd(m, i).wait_send()
        return carry

    lax.fori_loop(0, n_own, drain_w, 0)

    def drain_c(k, carry):
        for kind in range(3):
            send_x(kind, k).wait_send()
            send_y(kind, k).wait_send()
        return carry

    lax.fori_loop(0, n_chunk, drain_c, 0)
    for cp in (tok_x, tok_y, tok_d, *g_copies):
        cp.wait_send()


def solution(mesh):
    ep_size = mesh.shape["ep"]
    row_spec = P(("rep", "ep", "fsdp"), None)

    def device_step(tokens, expert_idx, gates, w_gate, w_up, w_down):
        rows, top_k = expert_idx.shape
        n_local, half_w, ffn = w_gate.shape
        width = tokens.shape[1]
        n_own = n_local // 2
        num_experts = n_local * ep_size
        capacity = (2 * rows * top_k + num_experts - 1) // num_experts
        half = rows // 2
        chunk = 64
        n_chunk = half // chunk
        dma = pltpu.SemaphoreType.DMA
        hbm = pl.BlockSpec(memory_space=pl.ANY)
        vmem = pl.BlockSpec(memory_space=pltpu.VMEM)
        return pl.pallas_call(
            functools.partial(moe_kernel, num_experts, capacity, chunk),
            out_shape=jax.ShapeDtypeStruct((rows, width), jnp.bfloat16),
            in_specs=[hbm, vmem, vmem, hbm, hbm, hbm],
            out_specs=vmem,
            scratch_shapes=[
                pltpu.VMEM((4 * rows, width), jnp.bfloat16),
                pltpu.VMEM((3, n_local, 2, half_w, ffn), jnp.bfloat16),
                pltpu.VMEM((4 * rows, width), jnp.float32),
                pltpu.VMEM((2, 4 * rows, ffn), jnp.bfloat16),
                pltpu.VMEM((128, rows), jnp.float32),
                pltpu.VMEM((3, n_local, rows), jnp.float32),
                pltpu.VMEM((4, rows, 128), jnp.float32),
                pltpu.VMEM((3, half, width), jnp.float32),
                pltpu.VMEM((3, half, width), jnp.float32),
                dma, dma((3,)), dma((3,)), dma((3,)), dma((3,)),
                dma((3, n_own)), dma((3, n_own)), dma((3, n_own)),
                dma((3, n_own)), dma((3, n_own)), dma((3, n_own)), dma((3, n_own)),
                dma((3, n_chunk)), dma((3, n_chunk)), dma((3, n_chunk)), dma((3, n_chunk)),
            ],
            compiler_params=pltpu.CompilerParams(collective_id=0, has_side_effects=True, vmem_limit_bytes=67_043_328),
        )(tokens, expert_idx, gates, w_gate, w_up, w_down)

    return jax.shard_map(device_step, mesh=mesh, in_specs=(row_spec, row_spec, row_spec, P("ep", "fsdp", None), P("ep", "fsdp", None), P("ep", None, "fsdp")), out_specs=row_spec, check_vma=False)
```

```python
import functools

import jax
import jax.numpy as jnp
from jax import lax
from jax.experimental import pallas as pl
from jax.experimental.pallas import tpu as pltpu
from jax.sharding import PartitionSpec as P

MESH = pl.DeviceIdType.MESH
OWN, XN, YN, DG = 0, 1, 2, 3


def moe_kernel(num_experts, capacity, chunk, tokens_hbm, idx_ref, gates_ref, wg_hbm, wu_hbm, wd_hbm, out_ref,
               tok, w, acc, hid, gt_send, gt_recv, gcol, rx, ry,
               loc_tok_sem, tok_send, tok_recv, g_send, g_recv_sem, loc_sem, ys_sem, yr_sem,
               po_s, po_r, pf_s, pf_r, cx_s, cx_r, cy_s, cy_r):
    rows, width = out_ref.shape
    n_local = wg_hbm.shape[0]
    n_own = n_local // 2
    half_w = width // 2
    n_chunk = rows // chunk
    ep = lax.axis_index("ep")
    y = lax.axis_index("fsdp")
    c = lax.rem(ep, 2)
    x = ep // 2
    oy = 1 - y
    x_dev = {"ep": lax.rem(ep + 2, 4), "fsdp": y}
    y_dev = {"ep": ep, "fsdp": oy}
    d_dev = {"ep": lax.rem(ep + 2, 4), "fsdp": oy}
    p_dev = {"ep": ep + 1 - 2 * c, "fsdp": y}
    w_hbm = (wg_hbm, wu_hbm, wd_hbm)

    def remote(src, dst, s, r, dev):
        return pltpu.make_async_remote_copy(src_ref=src, dst_ref=dst, send_sem=s, recv_sem=r, device_id=dev, device_id_type=MESH)

    def span(start, n):
        return pl.ds(pl.multiple_of(start, chunk), n)

    def block(b):
        return tok.at[pl.ds(b * rows, rows)]

    barrier = pltpu.get_barrier_semaphore()
    for dev in (x_dev, y_dev, d_dev, p_dev):
        pl.semaphore_signal(barrier, inc=1, device_id=dev, device_id_type=MESH)
    pl.semaphore_wait(barrier, 4)

    tok_y = remote(tokens_hbm, block(YN), tok_send.at[0], tok_recv.at[0], y_dev)
    tok_x = remote(tokens_hbm, block(XN), tok_send.at[1], tok_recv.at[1], x_dev)
    tok_d = remote(block(YN), block(DG), tok_send.at[2], tok_recv.at[2], x_dev)
    tok_l = pltpu.make_async_copy(tokens_hbm, block(OWN), loc_tok_sem)
    tok_y.start()
    tok_x.start()
    tok_l.start()

    row = lax.broadcasted_iota(jnp.int32, (num_experts, 1), 0)
    dest, slot = row // n_local, lax.rem(row, n_local)
    dx, dy = lax.rem(dest, 2), dest // 2
    ex = x + dx - 2 * x * dx
    ey = y + dy - 2 * y * dy
    sc = slot // n_own
    ec = c + sc - 2 * c * sc
    expert = (2 * ex + ec) * n_local + ey * n_own + lax.rem(slot, n_own)
    dense = jnp.zeros((num_experts, rows), jnp.float32)
    chosen = jnp.zeros((num_experts, rows), jnp.float32)
    for j in range(idx_ref.shape[0]):
        hit = idx_ref[j:j + 1, :] == expert
        dense = jnp.where(hit, gates_ref[j:j + 1, :], dense)
        chosen = jnp.where(hit, 1.0, chosen)
    before = lax.broadcasted_iota(jnp.int32, (rows, rows), 0) < lax.broadcasted_iota(jnp.int32, (rows, rows), 1)
    taken = jnp.dot(chosen.astype(jnp.bfloat16), before.astype(jnp.bfloat16), preferred_element_type=jnp.float32)
    dense = jnp.where(taken < float(capacity), dense, 0.0)
    gt_send[...] = dense
    g_copies = []
    for k, (b, dev) in enumerate(((XN, x_dev), (YN, y_dev), (DG, d_dev))):
        cp = remote(gt_send.at[pl.ds(b * n_local, n_local)], gt_recv.at[k], g_send.at[k], g_recv_sem.at[k], dev)
        cp.start()
        g_copies.append(cp)

    def local_w(m, i):
        return pltpu.make_async_copy(w_hbm[m].at[y * n_own + i], w.at[m, i, y], loc_sem.at[m, i])

    def send_w(m, i):
        return remote(w_hbm[m].at[oy * n_own + i], w.at[m, i, y], ys_sem.at[m, i], yr_sem.at[m, i], y_dev)

    def arrived_w(m, i):
        return remote(w_hbm[m].at[oy * n_own + i], w.at[m, i, oy], ys_sem.at[m, i], yr_sem.at[m, i], y_dev)

    def partner_own(m, i):
        return remote(w_hbm[m].at[y * n_own + i], w.at[m, n_own + i, y], po_s.at[m, i], po_r.at[m, i], p_dev)

    def partner_fwd(m, i):
        return remote(w.at[m, i, oy], w.at[m, n_own + i, oy], pf_s.at[m, i], pf_r.at[m, i], p_dev)

    for i in range(n_own):
        for m in range(2):
            send_w(m, i).start()
    for i in range(n_own):
        send_w(2, i).start()
    for i in range(n_own):
        for m in range(3):
            local_w(m, i).start()
            partner_own(m, i).start()

    def clear(k, carry):
        for part in range(2):
            acc[part, span(k * chunk, chunk), :] = jnp.zeros((chunk, half_w), jnp.float32)
        return carry

    lax.fori_loop(0, 4 * n_chunk, clear, 0)

    def column_gates(b, g):
        gcol[pl.ds(b * rows, rows), :] = jnp.concatenate([g, jnp.zeros((128 - n_local, rows), jnp.float32)], axis=0).T

    column_gates(OWN, gt_send[0:n_local, :])
    tok_y.wait_recv()
    tok_d.start()
    for k, b in enumerate((XN, YN, DG)):
        g_copies[k].wait_recv()
        column_gates(b, gt_recv[k])

    tok_l.wait()
    tok_x.wait_recv()
    tok_d.wait_recv()

    lane = lax.broadcasted_iota(jnp.int32, (1, 128), 1)

    def gate_up(s, start, n):
        at = span(start, n)
        r = tok[at, :]
        a = jnp.dot(r, w[0, s].reshape(width, w.shape[-1]), preferred_element_type=jnp.float32)
        u = jnp.dot(r, w[1, s].reshape(width, w.shape[-1]), preferred_element_type=jnp.float32)
        hid[s, at, :] = (a * jax.nn.sigmoid(a) * u).astype(jnp.bfloat16)

    def weighted(s, start, n, part):
        at = span(start, n)
        g = jnp.sum(jnp.where(lane == s, gcol[at, :], 0.0), axis=1, keepdims=True)
        o = jnp.dot(hid[s, at, :], w[2, s, part], preferred_element_type=jnp.float32).astype(jnp.bfloat16).astype(jnp.float32)
        return jnp.where(g != 0.0, g * o, 0.0)

    def down(s, part):
        def step(b, carry):
            at = span(b * rows, rows)
            acc[part, at, :] = acc[part, at, :] + weighted(s, b * rows, rows, part)
            return carry

        lax.fori_loop(0, 4, step, 0)

    def arrive(m, i):
        arrived_w(m, i).wait_recv()
        partner_fwd(m, i).start()

    def round_one(i, carry):
        for m in range(2):
            arrive(m, i)
            local_w(m, i).wait()
        local_w(2, i).wait()

        def both(s):
            def step(b, carry):
                at = span(b * rows, rows)
                gate_up(s, b * rows, rows)
                acc[y, at, :] = acc[y, at, :] + weighted(s, b * rows, rows, y)
                return carry

            lax.fori_loop(0, 4, step, 0)

        both(i)
        for m in range(2):
            partner_own(m, i).wait_recv()
            partner_fwd(m, i).wait_recv()
        partner_own(2, i).wait_recv()
        both(n_own + i)
        return carry

    lax.fori_loop(0, n_own - 1, round_one, 0)

    last = n_own - 1
    tile = 2 * chunk
    n_tile = rows // tile

    def tile_of(part, b, k):
        return acc.at[part, span(b * rows + k * tile, tile)]

    def send_x(kind, k):
        part = y if kind < 2 else oy
        return remote(tile_of(part, (DG, XN)[kind % 2], k), rx.at[kind, span(k * tile, tile)], cx_s.at[kind, k], cx_r.at[kind, k], x_dev)

    def send_y(kind, k):
        part = y if kind == 0 else oy
        return remote(tile_of(part, YN, k), ry.at[kind, span(k * tile, tile)], cy_s.at[kind, k], cy_r.at[kind, k], y_dev)

    def add_tile(part, b, k, got):
        at = span(b * rows + k * tile, tile)
        acc[part, at, :] = acc[part, at, :] + got[span(k * tile, tile), :]

    def finish(part, start, n):
        at = span(start, n)
        acc[part, at, :] = (acc[part, at, :] + weighted(last, start, n, part)) + weighted(n_own + last, start, n, part)

    for m in range(2):
        arrive(m, last)
        local_w(m, last).wait()
    local_w(2, last).wait()
    for m in range(2):
        partner_own(m, last).wait_recv()
        partner_fwd(m, last).wait_recv()
    partner_own(2, last).wait_recv()

    def close_one(b, k, n):
        start = b * rows + k * n
        gate_up(last, start, n)
        gate_up(n_own + last, start, n)
        finish(y, start, n)

    for kind, b in enumerate((DG, XN)):
        def step(k, carry, kind=kind, b=b):
            close_one(b, k, tile)
            send_x(kind, k).start()
            return carry

        lax.fori_loop(0, n_tile, step, 0)
    close_one(YN, 0, rows)
    close_one(OWN, 0, rows)

    def round_two(i, carry):
        arrive(2, i)
        down(i, oy)
        partner_fwd(2, i).wait_recv()
        down(n_own + i, oy)
        return carry

    lax.fori_loop(0, n_own - 1, round_two, 0)

    def pass_one(k, carry):
        send_x(0, k).wait_recv()
        add_tile(y, YN, k, rx.at[0])
        send_y(0, k).start()
        return carry

    lax.fori_loop(0, n_tile, pass_one, 0)

    arrive(2, last)
    partner_fwd(2, last).wait_recv()
    for kind, b in ((2, DG), (3, XN)):
        def step(k, carry, kind=kind, b=b):
            finish(oy, b * rows + k * tile, tile)
            send_x(kind, k).start()
            return carry

        lax.fori_loop(0, n_tile, step, 0)
    finish(oy, YN * rows, rows)
    finish(oy, OWN * rows, rows)

    def pass_two(k, carry):
        send_x(2, k).wait_recv()
        add_tile(oy, YN, k, rx.at[2])
        send_y(1, k).start()
        return carry

    lax.fori_loop(0, n_tile, pass_two, 0)

    def add_first(k, carry):
        send_x(1, k).wait_recv()
        add_tile(y, OWN, k, rx.at[1])
        send_y(0, k).wait_recv()
        add_tile(oy, OWN, k, ry.at[0])
        return carry

    lax.fori_loop(0, n_tile, add_first, 0)

    def last_add(k, carry):
        at = span(k * tile, tile)
        send_y(1, k).wait_recv()
        acc[y, at, :] = acc[y, at, :] + ry[1, at, :]
        send_x(3, k).wait_recv()
        acc[oy, at, :] = acc[oy, at, :] + rx[3, at, :]
        for part in range(2):
            cols = pl.ds(part * half_w, half_w)
            out_ref[at, cols] = (tok[at, cols].astype(jnp.float32) + acc[part, at, :]).astype(out_ref.dtype)
        return carry

    lax.fori_loop(0, n_tile, last_add, 0)

    def drain_w(i, carry):
        for m in range(3):
            send_w(m, i).wait_send()
            partner_own(m, i).wait_send()
            partner_fwd(m, i).wait_send()
        return carry

    lax.fori_loop(0, n_own, drain_w, 0)

    def drain_c(k, carry):
        for kind in range(4):
            send_x(kind, k).wait_send()
        for kind in range(2):
            send_y(kind, k).wait_send()
        return carry

    lax.fori_loop(0, n_tile, drain_c, 0)
    for cp in (tok_x, tok_y, tok_d, *g_copies):
        cp.wait_send()


def solution(mesh):
    ep_size = mesh.shape["ep"]
    row_spec = P(("rep", "ep", "fsdp"), None)

    def device_step(tokens, expert_idx, gates, w_gate, w_up, w_down):
        rows, top_k = expert_idx.shape
        n_local, half_w, ffn = w_gate.shape
        width = tokens.shape[1]
        n_own = n_local // 2
        num_experts = n_local * ep_size
        capacity = (2 * rows * top_k + num_experts - 1) // num_experts
        chunk = 64
        n_tile = rows // (2 * chunk)
        dma = pltpu.SemaphoreType.DMA
        hbm = pl.BlockSpec(memory_space=pl.ANY)
        vmem = pl.BlockSpec(memory_space=pltpu.VMEM)
        return pl.pallas_call(
            functools.partial(moe_kernel, num_experts, capacity, chunk),
            out_shape=jax.ShapeDtypeStruct((rows, width), jnp.bfloat16),
            in_specs=[hbm, vmem, vmem, hbm, hbm, hbm],
            out_specs=vmem,
            scratch_shapes=[
                pltpu.VMEM((4 * rows, width), jnp.bfloat16),
                pltpu.VMEM((3, n_local, 2, half_w, ffn), jnp.bfloat16),
                pltpu.VMEM((2, 4 * rows, half_w), jnp.float32),
                pltpu.VMEM((n_local, 4 * rows, ffn), jnp.bfloat16),
                pltpu.VMEM((num_experts, rows), jnp.float32),
                pltpu.VMEM((3, n_local, rows), jnp.float32),
                pltpu.VMEM((4 * rows, 128), jnp.float32),
                pltpu.VMEM((4, rows, half_w), jnp.float32),
                pltpu.VMEM((2, rows, half_w), jnp.float32),
                dma, dma((3,)), dma((3,)), dma((3,)), dma((3,)),
                dma((3, n_own)), dma((3, n_own)), dma((3, n_own)),
                dma((3, n_own)), dma((3, n_own)), dma((3, n_own)), dma((3, n_own)),
                dma((4, n_tile)), dma((4, n_tile)), dma((2, n_tile)), dma((2, n_tile)),
            ],
            compiler_params=pltpu.CompilerParams(collective_id=0, has_side_effects=True, vmem_limit_bytes=67_043_328),
        )(tokens, expert_idx.T, gates.T, w_gate, w_up, w_down)

    return jax.shard_map(device_step, mesh=mesh, in_specs=(row_spec, row_spec, row_spec, P("ep", "fsdp", None), P("ep", "fsdp", None), P("ep", None, "fsdp")), out_specs=row_spec, check_vma=False)
```

```python
import functools

import jax
import jax.numpy as jnp
from jax import lax
from jax.experimental import pallas as pl
from jax.experimental.pallas import tpu as pltpu
from jax.sharding import PartitionSpec as P

MESH = pl.DeviceIdType.MESH
OWN, XN, YN, DG = 0, 1, 2, 3


def moe_kernel(num_experts, capacity, chunk, spill_rows, tokens_hbm, idx_hbm, gates_hbm, wg_hbm, wu_hbm, wd_hbm, out_hbm,
               idx_ref, gates_ref, tok, w, acc, hid, gt_send, gt_recv, gcol, rx, ry, ry_spill,
               small_sem, out_sem, loc_tok_sem, tok_send, tok_recv, g_send, g_recv_sem, loc_sem, ys_sem, yr_sem,
               po_s, po_r, pf_s, pf_r, ds_sem, dr_sem, df_s, df_r, cx_s, cx_r, cy_s, cy_r, spill_s, spill_r):
    rows, width = out_hbm.shape
    n_local = wg_hbm.shape[0]
    n_own = n_local // 2
    half_w = width // 2
    group = half_w // 2
    n_chunk = rows // chunk
    ep = lax.axis_index("ep")
    y = lax.axis_index("fsdp")
    c = lax.rem(ep, 2)
    x = ep // 2
    oy = 1 - y
    x_dev = {"ep": lax.rem(ep + 2, 4), "fsdp": y}
    y_dev = {"ep": ep, "fsdp": oy}
    p_dev = {"ep": ep + 1 - 2 * c, "fsdp": y}
    w_hbm = (wg_hbm, wu_hbm, wd_hbm)

    def remote(src, dst, s, r, dev):
        return pltpu.make_async_remote_copy(src_ref=src, dst_ref=dst, send_sem=s, recv_sem=r, device_id=dev, device_id_type=MESH)

    def span(start, n):
        return pl.ds(pl.multiple_of(start, 16), n)

    def block(b):
        return tok.at[pl.ds(b * rows, rows)]

    idx_in = pltpu.make_async_copy(idx_hbm, idx_ref, small_sem.at[0])
    gates_in = pltpu.make_async_copy(gates_hbm, gates_ref, small_sem.at[1])
    idx_in.start()
    gates_in.start()
    barrier = pltpu.get_barrier_semaphore()
    for dev in (y_dev, x_dev, p_dev):
        pl.semaphore_signal(barrier, inc=1, device_id=dev, device_id_type=MESH)
    pl.semaphore_wait(barrier, 3)

    tok_y = remote(tokens_hbm, block(YN), tok_send.at[0], tok_recv.at[0], y_dev)
    tok_x = remote(tokens_hbm, block(XN), tok_send.at[1], tok_recv.at[1], x_dev)
    tok_d = remote(block(YN), block(DG), tok_send.at[2], tok_recv.at[2], x_dev)
    tok_l = pltpu.make_async_copy(tokens_hbm, block(OWN), loc_tok_sem)
    tok_y.start()
    tok_x.start()
    tok_l.start()

    row = lax.broadcasted_iota(jnp.int32, (num_experts, 1), 0)
    dest, slot = row // n_local, lax.rem(row, n_local)
    dx, dy = lax.rem(dest, 2), dest // 2
    ex = x + dx - 2 * x * dx
    ey = y + dy - 2 * y * dy
    sc = slot // n_own
    ec = c + sc - 2 * c * sc
    expert = (2 * ex + ec) * n_local + ey * n_own + lax.rem(slot, n_own)
    idx_in.wait()
    gates_in.wait()
    dense = jnp.zeros((num_experts, rows), jnp.float32)
    chosen = jnp.zeros((num_experts, rows), jnp.float32)
    for j in range(idx_ref.shape[0]):
        hit = idx_ref[j:j + 1, :] == expert
        dense = jnp.where(hit, gates_ref[j:j + 1, :], dense)
        chosen = jnp.where(hit, 1.0, chosen)
    before = lax.broadcasted_iota(jnp.int32, (rows, rows), 0) < lax.broadcasted_iota(jnp.int32, (rows, rows), 1)
    taken = jnp.dot(chosen.astype(jnp.bfloat16), before.astype(jnp.bfloat16), preferred_element_type=jnp.float32)
    dense = jnp.where(taken < float(capacity), dense, 0.0)
    gt_send[...] = dense
    g_x = remote(gt_send.at[pl.ds(XN * n_local, n_local)], gt_recv.at[pl.ds(0, n_local)], g_send.at[0], g_recv_sem.at[0], x_dev)
    g_y = remote(gt_send.at[pl.ds(YN * n_local, 2 * n_local)], gt_recv.at[pl.ds(n_local, 2 * n_local)], g_send.at[1], g_recv_sem.at[1], y_dev)
    g_d = remote(gt_recv.at[pl.ds(2 * n_local, n_local)], gt_recv.at[pl.ds(3 * n_local, n_local)], g_send.at[2], g_recv_sem.at[2], x_dev)
    g_y.start()
    g_x.start()

    def local_w(m, i):
        return pltpu.make_async_copy(w_hbm[m].at[y * n_own + i], w.at[m, i, y], loc_sem.at[m, i])

    def send_w(m, i):
        return remote(w_hbm[m].at[oy * n_own + i], w.at[m, i, y], ys_sem.at[m, i], yr_sem.at[m, i], y_dev)

    def arrived_w(m, i):
        return remote(w_hbm[m].at[oy * n_own + i], w.at[m, i, oy], ys_sem.at[m, i], yr_sem.at[m, i], y_dev)

    def partner_own(m, i):
        return remote(w_hbm[m].at[y * n_own + i], w.at[m, n_own + i, y], po_s.at[m, i], po_r.at[m, i], p_dev)

    def partner_fwd(m, i):
        return remote(w.at[m, i, oy], w.at[m, n_own + i, oy], pf_s.at[m, i], pf_r.at[m, i], p_dev)

    def down_half(slot, part, g):
        return w.at[2, slot, part, :, pl.ds(g * group, group)]

    def send_d(g, i):
        return remote(wd_hbm.at[oy * n_own + i, :, pl.ds(g * group, group)], down_half(i, y, g), ds_sem.at[g, i], dr_sem.at[g, i], y_dev)

    def arrived_d(g, i):
        return remote(wd_hbm.at[oy * n_own + i, :, pl.ds(g * group, group)], down_half(i, oy, g), ds_sem.at[g, i], dr_sem.at[g, i], y_dev)

    def fwd_d(g, i):
        return remote(down_half(i, oy, g), down_half(n_own + i, oy, g), df_s.at[g, i], df_r.at[g, i], p_dev)

    for i in range(n_own):
        for m in range(2):
            send_w(m, i).start()
    for g in range(2):
        for i in range(n_own):
            send_d(g, i).start()
    for i in range(n_own):
        for m in range(3):
            local_w(m, i).start()
            partner_own(m, i).start()

    def clear(k, carry):
        for part in range(2):
            acc[part, span(k * chunk, chunk), :] = jnp.zeros((chunk, half_w), jnp.float32)
        return carry

    lax.fori_loop(0, 4 * n_chunk, clear, 0)

    def column_gates(b, g):
        gcol[pl.ds(b * rows, rows), :] = jnp.concatenate([g, jnp.zeros((128 - n_local, rows), jnp.float32)], axis=0).T

    column_gates(OWN, gt_send[0:n_local, :])
    tok_y.wait_recv()
    tok_d.start()
    g_y.wait_recv()
    g_d.start()
    for k, (b, cp) in enumerate(((XN, g_x), (YN, None), (None, None), (DG, g_d))):
        if cp is not None:
            cp.wait_recv()
        if b is not None:
            column_gates(b, gt_recv[k * n_local:(k + 1) * n_local, :])

    tok_l.wait()
    tok_x.wait_recv()
    tok_d.wait_recv()

    lane = lax.broadcasted_iota(jnp.int32, (1, 128), 1)

    def gate_up(s, start, n):
        at = span(start, n)
        r = tok[at, :]
        a = jnp.dot(r, w[0, s].reshape(width, w.shape[-1]), preferred_element_type=jnp.float32)
        u = jnp.dot(r, w[1, s].reshape(width, w.shape[-1]), preferred_element_type=jnp.float32)
        hid[s, at, :] = (a * jax.nn.sigmoid(a) * u).astype(jnp.bfloat16)

    def weighted(s, start, n, part, col=0, n_col=half_w):
        at = span(start, n)
        g = jnp.sum(jnp.where(lane == s, gcol[at, :], 0.0), axis=1, keepdims=True)
        o = jnp.dot(hid[s, at, :], w[2, s, part, :, pl.ds(col, n_col)], preferred_element_type=jnp.float32).astype(jnp.bfloat16).astype(jnp.float32)
        return jnp.where(g != 0.0, g * o, 0.0)

    def down(s, g):
        cols = pl.ds(g * group, group)

        def step(b, carry):
            at = span(b * rows, rows)
            acc[oy, at, cols] = acc[oy, at, cols] + weighted(s, b * rows, rows, oy, g * group, group)
            return carry

        lax.fori_loop(0, 4, step, 0)

    def arrive(m, i):
        arrived_w(m, i).wait_recv()
        partner_fwd(m, i).start()

    def round_one(i, carry):
        for m in range(2):
            arrive(m, i)
            local_w(m, i).wait()
        local_w(2, i).wait()

        def both(s):
            def step(b, carry):
                at = span(b * rows, rows)
                gate_up(s, b * rows, rows)
                acc[y, at, :] = acc[y, at, :] + weighted(s, b * rows, rows, y)
                return carry

            lax.fori_loop(0, 4, step, 0)

        both(i)
        for m in range(2):
            partner_own(m, i).wait_recv()
            partner_fwd(m, i).wait_recv()
        partner_own(2, i).wait_recv()
        both(n_own + i)
        return carry

    lax.fori_loop(0, n_own - 1, round_one, 0)

    last = n_own - 1
    tile = 2 * chunk
    n_tile = rows // tile
    kept = rows - spill_rows
    starts = [0, tile // 2, *range(tile, kept, tile)]
    pieces = [(a, b - a) for a, b in zip(starts, [*starts[1:], kept])]
    n_first = len(pieces)

    def part_of(part, b, start, n):
        return acc.at[part, span(b * rows + start, n)]

    def send_x(kind, k):
        start, n = pieces[k] if kind == 0 else (k * tile, tile)
        return remote(part_of(y, (DG, XN)[kind], start, n), rx.at[kind, span(start, n)], cx_s.at[kind, k], cx_r.at[kind, k], x_dev)

    def send_xg(kind, g, k):
        cols = pl.ds(g * group, group)
        sem = 2 + 2 * kind + g
        return remote(acc.at[oy, span((DG, XN)[kind] * rows + k * tile, tile), cols], rx.at[2 + kind, span(k * tile, tile), cols],
                      cx_s.at[sem, k], cx_r.at[sem, k], x_dev)

    def send_y(k):
        return remote(part_of(y, YN, k * tile, tile), ry.at[0, span(k * tile, tile)], cy_s.at[0, k], cy_r.at[0, k], y_dev)

    def send_yg(g, k):
        cols = pl.ds(g * group, group)
        return remote(acc.at[oy, span(YN * rows + k * tile, tile), cols], ry.at[1, span(k * tile, tile), cols],
                      cy_s.at[1 + g, k], cy_r.at[1 + g, k], y_dev)

    spill = remote(part_of(y, DG, kept, spill_rows), ry_spill, spill_s, spill_r, y_dev)

    def add_rows(part, b, start, n, got, col=0, n_col=half_w):
        at, cols = span(b * rows + start, n), pl.ds(col, n_col)
        acc[part, at, cols] = acc[part, at, cols] + got[:, cols]

    def finish(part, start, n, col=0, n_col=half_w):
        at, cols = span(start, n), pl.ds(col, n_col)
        first = acc[part, at, cols] + weighted(last, start, n, part, col, n_col)
        acc[part, at, cols] = first + weighted(n_own + last, start, n, part, col, n_col)

    for m in range(2):
        arrive(m, last)
        local_w(m, last).wait()
    local_w(2, last).wait()
    for m in range(2):
        partner_own(m, last).wait_recv()
        partner_fwd(m, last).wait_recv()
    partner_own(2, last).wait_recv()

    def close_one(b, start, n):
        start = b * rows + start
        gate_up(last, start, n)
        gate_up(n_own + last, start, n)
        finish(y, start, n)

    def x_one(k, carry):
        close_one(XN, k * tile, tile)
        send_x(1, k).start()
        return carry

    for k, (start, n) in enumerate(pieces):
        close_one(DG, start, n)
        send_x(0, k).start()
    close_one(DG, kept, spill_rows)
    spill.start()
    lax.fori_loop(0, n_tile, x_one, 0)
    close_one(YN, 0, rows)
    close_one(OWN, 0, rows)

    def arrive_d(g, i):
        arrived_d(g, i).wait_recv()
        fwd_d(g, i).start()

    def round_two(i, carry, g=0):
        arrive_d(g, i)
        down(i, g)
        fwd_d(g, i).wait_recv()
        down(n_own + i, g)
        return carry

    def close_two(g, b):
        finish(oy, b * rows, rows, g * group, group)

    lax.fori_loop(0, n_own - 1, functools.partial(round_two, g=0), 0)
    arrive_d(0, last)
    fwd_d(0, last).wait_recv()

    def diag_two(k, carry, g=0):
        finish(oy, DG * rows + k * tile, tile, g * group, group)
        send_xg(0, g, k).start()
        return carry

    lax.fori_loop(0, n_tile, functools.partial(diag_two, g=0), 0)
    for b in (XN, YN, OWN):
        close_two(0, b)

    for k, (start, n) in enumerate(pieces):
        send_x(0, k).wait_recv()
        add_rows(y, YN, start, n, rx.at[0, span(start, n)])
        if k > 0:
            send_y(k - 1).start()

    lax.fori_loop(0, n_own - 1, functools.partial(round_two, g=1), 0)
    arrive_d(1, last)
    fwd_d(1, last).wait_recv()
    lax.fori_loop(0, n_tile, functools.partial(diag_two, g=1), 0)
    spill.wait_recv()
    add_rows(oy, XN, kept, spill_rows, ry_spill)
    for k in range(n_tile):
        send_xg(1, 0, k).start()

    def x_two(k, carry):
        finish(oy, XN * rows + k * tile, tile, group, group)
        send_xg(1, 1, k).start()
        return carry

    lax.fori_loop(0, n_tile, x_two, 0)
    close_two(1, YN)
    for g in range(2):
        def pass_two(k, carry, g=g):
            send_xg(0, g, k).wait_recv()
            add_rows(oy, YN, k * tile, tile, rx.at[2, span(k * tile, tile)], g * group, group)
            send_yg(g, k).start()
            return carry

        lax.fori_loop(0, n_tile, pass_two, 0)
        if g == 0:
            close_two(1, OWN)

    def add_first(k, carry):
        at = span(k * tile, tile)
        send_x(1, k).wait_recv()
        add_rows(y, OWN, k * tile, tile, rx.at[1, at])
        send_y(k).wait_recv()
        add_rows(oy, OWN, k * tile, tile, ry.at[0, at])
        return carry

    def add_second(k, carry):
        at = span(k * tile, tile)
        send_yg(0, k).wait_recv()
        add_rows(y, OWN, k * tile, tile, ry.at[1, at], 0, group)
        send_xg(1, 0, k).wait_recv()
        add_rows(oy, OWN, k * tile, tile, rx.at[3, at], 0, group)
        return carry

    lax.fori_loop(0, n_tile, add_first, 0)
    lax.fori_loop(0, n_tile, add_second, 0)

    def result(k):
        return pltpu.make_async_copy(tok.at[span(k * tile, tile)], out_hbm.at[span(k * tile, tile)], out_sem.at[k])

    def last_add(k, carry):
        at = span(k * tile, tile)
        send_yg(1, k).wait_recv()
        add_rows(y, OWN, k * tile, tile, ry.at[1, at], group, group)
        send_xg(1, 1, k).wait_recv()
        add_rows(oy, OWN, k * tile, tile, rx.at[3, at], group, group)
        for part in range(2):
            cols = pl.ds(part * half_w, half_w)
            tok[at, cols] = (tok[at, cols].astype(jnp.float32) + acc[part, at, :]).astype(tok.dtype)
        result(k).start()
        return carry

    lax.fori_loop(0, n_tile, last_add, 0)

    def drain_w(i, carry):
        for m in range(3):
            partner_own(m, i).wait_send()
        for m in range(2):
            send_w(m, i).wait_send()
            partner_fwd(m, i).wait_send()
        for g in range(2):
            send_d(g, i).wait_send()
            fwd_d(g, i).wait_send()
        return carry

    lax.fori_loop(0, n_own, drain_w, 0)
    for k in range(n_first):
        send_x(0, k).wait_send()

    def drain_c(k, carry):
        send_x(1, k).wait_send()
        send_y(k).wait_send()
        for g in range(2):
            send_xg(0, g, k).wait_send()
            send_xg(1, g, k).wait_send()
            send_yg(g, k).wait_send()
        result(k).wait()
        return carry

    lax.fori_loop(0, n_tile, drain_c, 0)
    for cp in (spill, tok_x, tok_y, tok_d, g_x, g_y, g_d):
        cp.wait_send()


def solution(mesh):
    ep_size = mesh.shape["ep"]
    row_spec = P(("rep", "ep", "fsdp"), None)

    def device_step(tokens, expert_idx, gates, w_gate, w_up, w_down):
        rows, top_k = expert_idx.shape
        n_local, half_w, ffn = w_gate.shape
        width = tokens.shape[1]
        n_own = n_local // 2
        num_experts = n_local * ep_size
        capacity = (2 * rows * top_k + num_experts - 1) // num_experts
        chunk, spill_rows = 64, 32
        n_chunk, n_tile = rows // chunk, rows // (2 * chunk)
        dma = pltpu.SemaphoreType.DMA
        hbm = pl.BlockSpec(memory_space=pl.ANY)
        return pl.pallas_call(
            functools.partial(moe_kernel, num_experts, capacity, chunk, spill_rows),
            out_shape=jax.ShapeDtypeStruct((rows, width), jnp.bfloat16),
            in_specs=[hbm] * 6,
            out_specs=hbm,
            scratch_shapes=[
                pltpu.VMEM((top_k, rows), jnp.int32),
                pltpu.VMEM((top_k, rows), jnp.float32),
                pltpu.VMEM((4 * rows, width), jnp.bfloat16),
                pltpu.VMEM((3, n_local, 2, half_w, ffn), jnp.bfloat16),
                pltpu.VMEM((2, 4 * rows, half_w), jnp.float32),
                pltpu.VMEM((n_local, 4 * rows, ffn), jnp.bfloat16),
                pltpu.VMEM((num_experts, rows), jnp.float32),
                pltpu.VMEM((4 * n_local, rows), jnp.float32),
                pltpu.VMEM((4 * rows, 128), jnp.float32),
                pltpu.VMEM((4, rows, half_w), jnp.float32),
                pltpu.VMEM((2, rows, half_w), jnp.float32),
                pltpu.VMEM((spill_rows, half_w), jnp.float32),
                dma((2,)), dma((n_tile,)), dma, dma((3,)), dma((3,)), dma((3,)), dma((3,)),
                dma((3, n_own)), dma((3, n_own)), dma((3, n_own)),
                dma((3, n_own)), dma((3, n_own)), dma((2, n_own)), dma((2, n_own)),
                dma((2, n_own)), dma((2, n_own)), dma((2, n_own)), dma((2, n_own)),
                dma((6, n_tile + 1)), dma((6, n_tile + 1)), dma((3, n_tile)), dma((3, n_tile)), dma, dma,
            ],
            compiler_params=pltpu.CompilerParams(collective_id=0, has_side_effects=True, vmem_limit_bytes=67_043_328),
        )(tokens, expert_idx.T, gates.T, w_gate, w_up, w_down)

    return jax.shard_map(device_step, mesh=mesh, in_specs=(row_spec, row_spec, row_spec, P("ep", "fsdp", None), P("ep", "fsdp", None), P("ep", None, "fsdp")), out_specs=row_spec, check_vma=False)
```

```python
import functools

import jax
import jax.numpy as jnp
from jax import lax
from jax.experimental import pallas as pl
from jax.experimental.pallas import tpu as pltpu
from jax.sharding import PartitionSpec as P

MESH = pl.DeviceIdType.MESH
OWN, XN, YN, DG = 0, 1, 2, 3


def moe_kernel(num_experts, capacity, chunk, spill_rows, tokens_hbm, idx_hbm, gates_hbm, wg_hbm, wu_hbm, wd_hbm, out_hbm,
               idx_ref, gates_ref, tok, w, acc, hid, gt_send, gt_recv, gcol, rx, ry, ry_spill,
               small_sem, out_sem, loc_tok_sem, tok_send, tok_recv, g_send, g_recv_sem, loc_sem, ys_sem, yr_sem,
               po_s, po_r, pf_s, pf_r, ds_sem, dr_sem, df_s, df_r, cx_s, cx_r, cy_s, cy_r, spill_s, spill_r):
    rows, width = out_hbm.shape
    n_local = wg_hbm.shape[0]
    n_own = n_local // 2
    half_w = width // 2
    group = half_w // 2
    n_chunk = rows // chunk
    ep = lax.axis_index("ep")
    y = lax.axis_index("fsdp")
    c = lax.rem(ep, 2)
    x = ep // 2
    oy = 1 - y
    x_dev = {"ep": lax.rem(ep + 2, 4), "fsdp": y}
    y_dev = {"ep": ep, "fsdp": oy}
    p_dev = {"ep": ep + 1 - 2 * c, "fsdp": y}
    w_hbm = (wg_hbm, wu_hbm, wd_hbm)

    def remote(src, dst, s, r, dev):
        return pltpu.make_async_remote_copy(src_ref=src, dst_ref=dst, send_sem=s, recv_sem=r, device_id=dev, device_id_type=MESH)

    def span(start, n):
        return pl.ds(pl.multiple_of(start, 16), n)

    def block(b):
        return tok.at[pl.ds(b * rows, rows)]

    idx_in = pltpu.make_async_copy(idx_hbm, idx_ref, small_sem.at[0])
    gates_in = pltpu.make_async_copy(gates_hbm, gates_ref, small_sem.at[1])
    idx_in.start()
    gates_in.start()
    barrier = pltpu.get_barrier_semaphore()
    for dev in (y_dev, x_dev, p_dev):
        pl.semaphore_signal(barrier, inc=1, device_id=dev, device_id_type=MESH)
    pl.semaphore_wait(barrier, 3)

    tok_y = remote(tokens_hbm, block(YN), tok_send.at[0], tok_recv.at[0], y_dev)
    tok_x = remote(tokens_hbm, block(XN), tok_send.at[1], tok_recv.at[1], x_dev)
    tok_d = remote(block(YN), block(DG), tok_send.at[2], tok_recv.at[2], x_dev)
    tok_l = pltpu.make_async_copy(tokens_hbm, block(OWN), loc_tok_sem)
    tok_x.start()
    tok_l.start()

    @pl.when(c == 1)
    def _():
        tok_y.start()

    row = lax.broadcasted_iota(jnp.int32, (num_experts, 1), 0)
    dest, slot = row // n_local, lax.rem(row, n_local)
    dx, dy = lax.rem(dest, 2), dest // 2
    ex = x + dx - 2 * x * dx
    ey = y + dy - 2 * y * dy
    sc = slot // n_own
    ec = c + sc - 2 * c * sc
    expert = (2 * ex + ec) * n_local + ey * n_own + lax.rem(slot, n_own)
    idx_in.wait()
    gates_in.wait()
    dense = jnp.zeros((num_experts, rows), jnp.float32)
    chosen = jnp.zeros((num_experts, rows), jnp.float32)
    for j in range(idx_ref.shape[0]):
        hit = idx_ref[j:j + 1, :] == expert
        dense = jnp.where(hit, gates_ref[j:j + 1, :], dense)
        chosen = jnp.where(hit, 1.0, chosen)
    before = lax.broadcasted_iota(jnp.int32, (rows, rows), 0) < lax.broadcasted_iota(jnp.int32, (rows, rows), 1)
    taken = jnp.dot(chosen.astype(jnp.bfloat16), before.astype(jnp.bfloat16), preferred_element_type=jnp.float32)
    dense = jnp.where(taken < float(capacity), dense, 0.0)
    gt_send[...] = dense
    g_x = remote(gt_send.at[pl.ds(XN * n_local, n_local)], gt_recv.at[pl.ds(0, n_local)], g_send.at[0], g_recv_sem.at[0], x_dev)
    g_y = remote(gt_send.at[pl.ds(YN * n_local, 2 * n_local)], gt_recv.at[pl.ds(n_local, 2 * n_local)], g_send.at[1], g_recv_sem.at[1], y_dev)
    g_d = remote(gt_recv.at[pl.ds(2 * n_local, n_local)], gt_recv.at[pl.ds(3 * n_local, n_local)], g_send.at[2], g_recv_sem.at[2], x_dev)


    g_x.start()

    def local_w(m, i):
        return pltpu.make_async_copy(w_hbm[m].at[y * n_own + i], w.at[m, i, y], loc_sem.at[m, i])

    def send_w(m, i):
        return remote(w_hbm[m].at[oy * n_own + i], w.at[m, i, y], ys_sem.at[m, i], yr_sem.at[m, i], y_dev)

    def arrived_w(m, i):
        return remote(w_hbm[m].at[oy * n_own + i], w.at[m, i, oy], ys_sem.at[m, i], yr_sem.at[m, i], y_dev)

    def partner_own(m, i):
        return remote(w_hbm[m].at[y * n_own + i], w.at[m, n_own + i, y], po_s.at[m, i], po_r.at[m, i], p_dev)

    def partner_fwd(m, i):
        return remote(w.at[m, i, oy], w.at[m, n_own + i, oy], pf_s.at[m, i], pf_r.at[m, i], p_dev)

    def down_half(slot, part, g):
        return w.at[2, slot, part, :, pl.ds(g * group, group)]

    def send_d(g, i):
        return remote(wd_hbm.at[oy * n_own + i, :, pl.ds(g * group, group)], down_half(i, y, g), ds_sem.at[g, i], dr_sem.at[g, i], y_dev)

    def arrived_d(g, i):
        return remote(wd_hbm.at[oy * n_own + i, :, pl.ds(g * group, group)], down_half(i, oy, g), ds_sem.at[g, i], dr_sem.at[g, i], y_dev)

    def fwd_d(g, i):
        return remote(down_half(i, oy, g), down_half(n_own + i, oy, g), df_s.at[g, i], df_r.at[g, i], p_dev)

    def send_gate_up():
        for i in range(n_own):
            for m in range(2):
                send_w(m, i).start()

    @pl.when(c == 1)
    def _():
        g_y.start()
        send_gate_up()

    def send_down():
        for g in range(2):
            for i in range(n_own):
                send_d(g, i).start()

    for i in range(n_own):
        for m in range(3):
            local_w(m, i).start()
            partner_own(m, i).start()

    @pl.when(c == 0)
    def _():
        local_w(0, 0).wait()
        tok_y.start()
        g_y.start()
        send_gate_up()
        send_down()

    def clear(k, carry):
        for part in range(2):
            acc[part, span(k * chunk, chunk), :] = jnp.zeros((chunk, half_w), jnp.float32)
        return carry

    lax.fori_loop(0, 4 * n_chunk, clear, 0)

    def column_gates(b, g):
        gcol[pl.ds(b * rows, rows), :] = jnp.concatenate([g, jnp.zeros((128 - n_local, rows), jnp.float32)], axis=0).T

    column_gates(OWN, gt_send[0:n_local, :])
    tok_y.wait_recv()
    tok_d.start()
    g_y.wait_recv()
    g_d.start()
    for k, (b, cp) in enumerate(((XN, g_x), (YN, None), (None, None), (DG, g_d))):
        if cp is not None:
            cp.wait_recv()
        if b is not None:
            column_gates(b, gt_recv[k * n_local:(k + 1) * n_local, :])

    tok_l.wait()
    tok_x.wait_recv()
    tok_d.wait_recv()

    lane = lax.broadcasted_iota(jnp.int32, (1, 128), 1)

    def gate_up(s, start, n):
        at = span(start, n)
        r = tok[at, :]
        a = jnp.dot(r, w[0, s].reshape(width, w.shape[-1]), preferred_element_type=jnp.float32)
        u = jnp.dot(r, w[1, s].reshape(width, w.shape[-1]), preferred_element_type=jnp.float32)
        hid[s, at, :] = (a * jax.nn.sigmoid(a) * u).astype(jnp.bfloat16)

    def weighted(s, start, n, part, col=0, n_col=half_w):
        at = span(start, n)
        g = jnp.sum(jnp.where(lane == s, gcol[at, :], 0.0), axis=1, keepdims=True)
        o = jnp.dot(hid[s, at, :], w[2, s, part, :, pl.ds(col, n_col)], preferred_element_type=jnp.float32).astype(jnp.bfloat16).astype(jnp.float32)
        return jnp.where(g != 0.0, g * o, 0.0)

    def down(s, g):
        cols = pl.ds(g * group, group)

        def step(b, carry):
            at = span(b * rows, rows)
            acc[oy, at, cols] = acc[oy, at, cols] + weighted(s, b * rows, rows, oy, g * group, group)
            return carry

        lax.fori_loop(0, 4, step, 0)

    def arrive(m, i):
        arrived_w(m, i).wait_recv()
        partner_fwd(m, i).start()

    def round_one(i, carry):
        for m in range(2):
            arrive(m, i)

        @pl.when((i > 0) | (c == 1))
        def _():
            local_w(0, i).wait()

        local_w(1, i).wait()
        local_w(2, i).wait()

        def both(s):
            def step(b, carry):
                at = span(b * rows, rows)
                gate_up(s, b * rows, rows)
                acc[y, at, :] = acc[y, at, :] + weighted(s, b * rows, rows, y)
                return carry

            lax.fori_loop(0, 4, step, 0)

        both(i)
        for m in range(2):
            partner_own(m, i).wait_recv()
            partner_fwd(m, i).wait_recv()
        partner_own(2, i).wait_recv()
        both(n_own + i)
        return carry

    lax.fori_loop(0, n_own - 1, round_one, 0)

    last = n_own - 1
    tile = 2 * chunk
    kept = rows - spill_rows
    starts = [0, tile // 2, tile, 2 * tile]
    pieces = [(a, b - a) for a, b in zip(starts, [*starts[1:], kept])]
    n_first = len(pieces)
    whole = [(0, rows)]
    fine = [(0, rows - tile), (rows - tile, tile - 32), (rows - 32, 32)]

    x_pieces = {(DG, 0): pieces, (XN, 0): whole, (DG, 1): whole, (DG, 2): whole, (XN, 1): whole, (XN, 2): fine}
    y_pieces = (whole, whole, fine)
    x_places = {kind: n for n, kind in enumerate(x_pieces)}
    landing = {DG: 0, XN: 1}

    def sums(stage, b, start, n):
        at = span(b * rows + start, n)
        return acc.at[y, at] if stage == 0 else acc.at[oy, at, pl.ds((stage - 1) * group, group)]

    def landed(buffer, slot, stage, start, n):
        at = span(start, n)
        return buffer.at[slot, at] if stage == 0 else buffer.at[slot, at, pl.ds((stage - 1) * group, group)]

    def send_x(b, stage, k):
        start, n = x_pieces[b, stage][k]
        slot = landing[b] + (2 if stage else 0)
        sem = x_places[b, stage]
        return remote(sums(stage, b, start, n), landed(rx, slot, stage, start, n), cx_s.at[sem, k], cx_r.at[sem, k], x_dev)

    def send_y(stage, k):
        start, n = y_pieces[stage][k]
        return remote(sums(stage, YN, start, n), landed(ry, 1 if stage else 0, stage, start, n), cy_s.at[stage, k], cy_r.at[stage, k], y_dev)

    spill = remote(sums(0, DG, kept, spill_rows), ry_spill, spill_s, spill_r, y_dev)

    def add_rows(part, b, start, n, got, col=0, n_col=half_w):
        at, cols = span(b * rows + start, n), pl.ds(col, n_col)
        acc[part, at, cols] = acc[part, at, cols] + got[:, cols]

    def finish(part, start, n, col=0, n_col=half_w):
        at, cols = span(start, n), pl.ds(col, n_col)
        first = acc[part, at, cols] + weighted(last, start, n, part, col, n_col)
        acc[part, at, cols] = first + weighted(n_own + last, start, n, part, col, n_col)

    arrive(0, last)
    for m in range(3):
        local_w(m, last).wait()
        partner_own(m, last).wait_recv()
    partner_fwd(0, last).wait_recv()
    head_start, head = DG * rows, pieces[0][1]

    @pl.when(c == 1)
    def _():
        arrive(1, last)
        gate_up(last, head_start, head)
        partner_fwd(1, last).wait_recv()
        send_down()
        gate_up(n_own + last, head_start, head)

    @pl.when(c == 0)
    def _():
        partner_fwd(1, last).wait_recv()
        gate_up(n_own + last, head_start, head)
        arrive(1, last)
        gate_up(last, head_start, head)

    def close_one(b, start, n):
        start = b * rows + start
        gate_up(last, start, n)
        gate_up(n_own + last, start, n)
        finish(y, start, n)

    finish(y, head_start, head)
    send_x(DG, 0, 0).start()
    for k, (start, n) in enumerate(pieces[1:], 1):
        close_one(DG, start, n)
        send_x(DG, 0, k).start()
    close_one(DG, kept, spill_rows)
    spill.start()
    close_one(XN, 0, rows)
    send_x(XN, 0, 0).start()
    close_one(YN, 0, rows)
    close_one(OWN, 0, rows)

    def arrive_d(g, i):
        arrived_d(g, i).wait_recv()
        fwd_d(g, i).start()

    def round_two(i, carry, g=0):
        arrive_d(g, i)
        down(i, g)
        fwd_d(g, i).wait_recv()
        down(n_own + i, g)
        return carry

    def close_two(g, b):
        finish(oy, b * rows, rows, g * group, group)

    lax.fori_loop(0, n_own - 1, functools.partial(round_two, g=0), 0)
    arrive_d(0, last)
    fwd_d(0, last).wait_recv()

    def add_x(part, b, stage, k):
        start, n = x_pieces[b, stage][k]
        send_x(b, stage, k).wait_recv()
        slot = landing[b] + (2 if stage else 0)
        add_rows(part, YN if b == DG else OWN, start, n, rx.at[slot, span(start, n)], *columns(stage))

    def add_y(part, stage, k):
        start, n = y_pieces[stage][k]
        send_y(stage, k).wait_recv()
        add_rows(part, OWN, start, n, ry.at[1 if stage else 0, span(start, n)], *columns(stage))

    def columns(stage):
        return (0, half_w) if stage == 0 else ((stage - 1) * group, group)

    close_two(0, DG)
    send_x(DG, 1, 0).start()

    def others(b, carry):
        close_two(0, b)
        return carry

    lax.fori_loop(OWN, DG, others, 0)
    for k in range(n_first):
        add_x(y, DG, 0, k)
    send_y(0, 0).start()

    lax.fori_loop(0, n_own - 1, functools.partial(round_two, g=1), 0)
    arrive_d(1, last)
    fwd_d(1, last).wait_recv()
    close_two(1, DG)
    send_x(DG, 2, 0).start()
    spill.wait_recv()
    add_rows(oy, XN, kept, spill_rows, ry_spill)
    send_x(XN, 1, 0).start()
    close_two(1, XN)
    for k in range(len(fine)):
        send_x(XN, 2, k).start()
    close_two(1, YN)
    add_x(oy, DG, 1, 0)
    send_y(1, 0).start()
    close_two(1, OWN)
    add_x(oy, DG, 2, 0)
    for k in range(len(fine)):
        send_y(2, k).start()
    add_x(y, XN, 0, 0)
    add_y(oy, 0, 0)
    add_y(y, 1, 0)
    add_x(oy, XN, 1, 0)

    def result(k):
        start, n = fine[k]
        return pltpu.make_async_copy(tok.at[span(start, n)], out_hbm.at[span(start, n)], out_sem.at[k])

    for k, (start, n) in enumerate(fine):
        at = span(start, n)
        add_y(y, 2, k)
        add_x(oy, XN, 2, k)
        for part in range(2):
            cols = pl.ds(part * half_w, half_w)
            tok[at, cols] = (tok[at, cols].astype(jnp.float32) + acc[part, at, :]).astype(tok.dtype)
        result(k).start()

    def drain_w(i, carry):
        for m in range(3):
            partner_own(m, i).wait_send()
        for m in range(2):
            send_w(m, i).wait_send()
            partner_fwd(m, i).wait_send()
        for g in range(2):
            send_d(g, i).wait_send()
            fwd_d(g, i).wait_send()
        return carry

    lax.fori_loop(0, n_own, drain_w, 0)
    for (b, stage), some in x_pieces.items():
        for k in range(len(some)):
            send_x(b, stage, k).wait_send()
    for stage, some in enumerate(y_pieces):
        for k in range(len(some)):
            send_y(stage, k).wait_send()
    for cp in (spill, tok_x, tok_y, tok_d, g_x, g_y, g_d):
        cp.wait_send()
    for k in range(len(fine)):
        result(k).wait()


def solution(mesh):
    ep_size = mesh.shape["ep"]
    row_spec = P(("rep", "ep", "fsdp"), None)

    def device_step(tokens, expert_idx, gates, w_gate, w_up, w_down):
        rows, top_k = expert_idx.shape
        n_local, half_w, ffn = w_gate.shape
        width = tokens.shape[1]
        n_own = n_local // 2
        num_experts = n_local * ep_size
        capacity = (2 * rows * top_k + num_experts - 1) // num_experts
        chunk, spill_rows = 64, 32
        dma = pltpu.SemaphoreType.DMA
        hbm = pl.BlockSpec(memory_space=pl.ANY)
        return pl.pallas_call(
            functools.partial(moe_kernel, num_experts, capacity, chunk, spill_rows),
            out_shape=jax.ShapeDtypeStruct((rows, width), jnp.bfloat16),
            in_specs=[hbm] * 6,
            out_specs=hbm,
            scratch_shapes=[
                pltpu.VMEM((top_k, rows), jnp.int32),
                pltpu.VMEM((top_k, rows), jnp.float32),
                pltpu.VMEM((4 * rows, width), jnp.bfloat16),
                pltpu.VMEM((3, n_local, 2, half_w, ffn), jnp.bfloat16),
                pltpu.VMEM((2, 4 * rows, half_w), jnp.float32),
                pltpu.VMEM((n_local, 4 * rows, ffn), jnp.bfloat16),
                pltpu.VMEM((num_experts, rows), jnp.float32),
                pltpu.VMEM((4 * n_local, rows), jnp.float32),
                pltpu.VMEM((4 * rows, 128), jnp.float32),
                pltpu.VMEM((4, rows, half_w), jnp.float32),
                pltpu.VMEM((2, rows, half_w), jnp.float32),
                pltpu.VMEM((spill_rows, half_w), jnp.float32),
                dma((2,)), dma((3,)), dma, dma((3,)), dma((3,)), dma((3,)), dma((3,)),
                dma((3, n_own)), dma((3, n_own)), dma((3, n_own)),
                dma((3, n_own)), dma((3, n_own)), dma((2, n_own)), dma((2, n_own)),
                dma((2, n_own)), dma((2, n_own)), dma((2, n_own)), dma((2, n_own)),
                dma((6, 4)), dma((6, 4)), dma((3, 3)), dma((3, 3)), dma, dma,
            ],
            compiler_params=pltpu.CompilerParams(collective_id=0, has_side_effects=True, vmem_limit_bytes=67_043_328),
        )(tokens, expert_idx.T, gates.T, w_gate, w_up, w_down)

    return jax.shard_map(device_step, mesh=mesh, in_specs=(row_spec, row_spec, row_spec, P("ep", "fsdp", None), P("ep", "fsdp", None), P("ep", None, "fsdp")), out_specs=row_spec, check_vma=False)
```

```python
import functools

import jax
import jax.numpy as jnp
from jax import lax
from jax.experimental import pallas as pl
from jax.experimental.pallas import tpu as pltpu
from jax.sharding import PartitionSpec as P

MESH = pl.DeviceIdType.MESH
OWN, XN, YN, DG = 0, 1, 2, 3


def moe_kernel(num_experts, capacity, chunk, late_rows, tokens_hbm, idx_hbm, gates_hbm, wg_hbm, wu_hbm, wd_hbm, out_hbm,
               idx_ref, gates_ref, tok, w, acc, hid, gt_send, gt_recv, gcol, gcol_x, rx, ry, o_out, o_in, go_sem,
               small_sem, out_sem, loc_tok_sem, tok_send, tok_recv, g_send, g_recv_sem, loc_sem, ys_sem, yr_sem,
               po_s, po_r, pf_s, pf_r, ds_sem, dr_sem, df_s, df_r, cx_s, cx_r, cy_s, cy_r, o_s, o_r):
    rows, width = out_hbm.shape
    n_local = wg_hbm.shape[0]
    n_own = n_local // 2
    half_w = width // 2
    group = half_w // 2
    n_chunk = rows // chunk
    ep = lax.axis_index("ep")
    y = lax.axis_index("fsdp")
    c = lax.rem(ep, 2)
    x = ep // 2
    oy = 1 - y
    x_dev = {"ep": lax.rem(ep + 2, 4), "fsdp": y}
    y_dev = {"ep": ep, "fsdp": oy}
    p_dev = {"ep": ep + 1 - 2 * c, "fsdp": y}
    w_hbm = (wg_hbm, wu_hbm, wd_hbm)

    def remote(src, dst, s, r, dev):
        return pltpu.make_async_remote_copy(src_ref=src, dst_ref=dst, send_sem=s, recv_sem=r, device_id=dev, device_id_type=MESH)

    def span(start, n):
        return pl.ds(pl.multiple_of(start, 16), n)

    def block(b):
        return tok.at[pl.ds(b * rows, rows)]

    idx_in = pltpu.make_async_copy(idx_hbm, idx_ref, small_sem.at[0])
    gates_in = pltpu.make_async_copy(gates_hbm, gates_ref, small_sem.at[1])
    idx_in.start()
    gates_in.start()
    barrier = pltpu.get_barrier_semaphore()
    for dev in (y_dev, x_dev, p_dev):
        pl.semaphore_signal(barrier, inc=1, device_id=dev, device_id_type=MESH)
    pl.semaphore_wait(barrier, 3)

    tok_y = remote(tokens_hbm, block(YN), tok_send.at[0], tok_recv.at[0], y_dev)
    tok_x = remote(tokens_hbm, block(XN), tok_send.at[1], tok_recv.at[1], x_dev)
    tok_d = remote(block(YN), block(DG), tok_send.at[2], tok_recv.at[2], x_dev)
    tok_l = pltpu.make_async_copy(tokens_hbm, block(OWN), loc_tok_sem)
    tok_x.start()
    tok_l.start()

    @pl.when(c == 1)
    def _():
        tok_y.start()

    row = lax.broadcasted_iota(jnp.int32, (num_experts, 1), 0)
    dest, slot = row // n_local, lax.rem(row, n_local)
    dx, dy = lax.rem(dest, 2), dest // 2
    ex = x + dx - 2 * x * dx
    ey = y + dy - 2 * y * dy
    sc = slot // n_own
    ec = c + sc - 2 * c * sc
    expert = (2 * ex + ec) * n_local + ey * n_own + lax.rem(slot, n_own)
    idx_in.wait()
    gates_in.wait()
    dense = jnp.zeros((num_experts, rows), jnp.float32)
    chosen = jnp.zeros((num_experts, rows), jnp.float32)
    for j in range(idx_ref.shape[0]):
        hit = idx_ref[j:j + 1, :] == expert
        dense = jnp.where(hit, gates_ref[j:j + 1, :], dense)
        chosen = jnp.where(hit, 1.0, chosen)
    before = lax.broadcasted_iota(jnp.int32, (rows, rows), 0) < lax.broadcasted_iota(jnp.int32, (rows, rows), 1)
    taken = jnp.dot(chosen.astype(jnp.bfloat16), before.astype(jnp.bfloat16), preferred_element_type=jnp.float32)
    dense = jnp.where(taken < float(capacity), dense, 0.0)
    gt_send[...] = dense
    g_x = remote(gt_send.at[pl.ds(XN * n_local, n_local)], gt_recv.at[pl.ds(0, n_local)], g_send.at[0], g_recv_sem.at[0], x_dev)
    g_y = remote(gt_send.at[pl.ds(YN * n_local, 2 * n_local)], gt_recv.at[pl.ds(n_local, 2 * n_local)], g_send.at[1], g_recv_sem.at[1], y_dev)
    g_d = remote(gt_recv.at[pl.ds(2 * n_local, n_local)], gt_recv.at[pl.ds(3 * n_local, n_local)], g_send.at[2], g_recv_sem.at[2], x_dev)


    g_x.start()

    def local_w(m, i):
        return pltpu.make_async_copy(w_hbm[m].at[y * n_own + i], w.at[m, i, y], loc_sem.at[m, i])

    def send_w(m, i):
        return remote(w_hbm[m].at[oy * n_own + i], w.at[m, i, y], ys_sem.at[m, i], yr_sem.at[m, i], y_dev)

    def arrived_w(m, i):
        return remote(w_hbm[m].at[oy * n_own + i], w.at[m, i, oy], ys_sem.at[m, i], yr_sem.at[m, i], y_dev)

    def partner_own(m, i):
        return remote(w_hbm[m].at[y * n_own + i], w.at[m, n_own + i, y], po_s.at[m, i], po_r.at[m, i], p_dev)

    def partner_fwd(m, i):
        return remote(w.at[m, i, oy], w.at[m, n_own + i, oy], pf_s.at[m, i], pf_r.at[m, i], p_dev)

    def down_half(slot, part, g):
        return w.at[2, slot, part, :, pl.ds(g * group, group)]

    def send_d(g, i):
        return remote(wd_hbm.at[oy * n_own + i, :, pl.ds(g * group, group)], down_half(i, y, g), ds_sem.at[g, i], dr_sem.at[g, i], y_dev)

    def arrived_d(g, i):
        return remote(wd_hbm.at[oy * n_own + i, :, pl.ds(g * group, group)], down_half(i, oy, g), ds_sem.at[g, i], dr_sem.at[g, i], y_dev)

    def fwd_d(g, i):
        return remote(down_half(i, oy, g), down_half(n_own + i, oy, g), df_s.at[g, i], df_r.at[g, i], p_dev)

    def send_gate_up():
        for i in range(n_own):
            for m in range(2):
                send_w(m, i).start()

    @pl.when(c == 1)
    def _():
        g_y.start()
        send_gate_up()

    def send_down():
        for g in range(2):
            for i in range(n_own):
                send_d(g, i).start()

    for i in range(n_own):
        for m in range(3):
            local_w(m, i).start()
            partner_own(m, i).start()

    def clear(k, carry):
        for part in range(2):
            acc[part, span(k * chunk, chunk), :] = jnp.zeros((chunk, half_w), jnp.float32)
        return carry

    lax.fori_loop(0, 4 * n_chunk, clear, 0)

    @pl.when(c == 1)
    def _():
        tok_y.wait_send()
        pl.semaphore_signal(go_sem, inc=1, device_id=p_dev, device_id_type=MESH)

    @pl.when(c == 0)
    def _():
        pl.semaphore_wait(go_sem, 1)
        tok_y.start()
        g_y.start()
        send_gate_up()
        send_down()

    def columns_of(g):
        return jnp.concatenate([g, jnp.zeros((128 - n_local, rows), jnp.float32)], axis=0).T

    def column_gates(b, g):
        gcol[pl.ds(b * rows, rows), :] = columns_of(g)

    column_gates(OWN, gt_send[0:n_local, :])
    gcol_x[...] = columns_of(gt_send[pl.ds(XN * n_local, n_local), :])
    tok_y.wait_recv()
    tok_d.start()
    g_y.wait_recv()
    g_d.start()
    for k, (b, cp) in enumerate(((XN, g_x), (YN, None), (None, None), (DG, g_d))):
        if cp is not None:
            cp.wait_recv()
        if b is not None:
            column_gates(b, gt_recv[k * n_local:(k + 1) * n_local, :])

    tok_l.wait()
    tok_x.wait_recv()
    tok_d.wait_recv()

    lane = lax.broadcasted_iota(jnp.int32, (1, 128), 1)

    def gate_up(s, start, n):
        at = span(start, n)
        r = tok[at, :]
        a = jnp.dot(r, w[0, s].reshape(width, w.shape[-1]), preferred_element_type=jnp.float32)
        u = jnp.dot(r, w[1, s].reshape(width, w.shape[-1]), preferred_element_type=jnp.float32)
        hid[s, at, :] = (a * jax.nn.sigmoid(a) * u).astype(jnp.bfloat16)

    def expert_rows(s, start, n, part, col=0, n_col=half_w):
        return jnp.dot(hid[s, span(start, n), :], w[2, s, part, :, pl.ds(col, n_col)], preferred_element_type=jnp.float32).astype(jnp.bfloat16)

    def scaled(gates, s, o):
        g = jnp.sum(jnp.where(lane == s, gates, 0.0), axis=1, keepdims=True)
        return jnp.where(g != 0.0, g * o.astype(jnp.float32), 0.0)

    def weighted(s, start, n, part, col=0, n_col=half_w):
        return scaled(gcol[span(start, n), :], s, expert_rows(s, start, n, part, col, n_col))

    def down(s, g):
        cols = pl.ds(g * group, group)

        def step(b, carry):
            at = span(b * rows, rows)
            acc[oy, at, cols] = acc[oy, at, cols] + weighted(s, b * rows, rows, oy, g * group, group)
            return carry

        lax.fori_loop(0, 4, step, 0)

    def arrive(m, i):
        arrived_w(m, i).wait_recv()
        partner_fwd(m, i).start()

    def await_own(i):
        for m in range(2):
            arrive(m, i)
        for m in range(3):
            local_w(m, i).wait()

    def await_partner(i):
        for m in range(3):
            partner_own(m, i).wait_recv()
        for m in range(2):
            partner_fwd(m, i).wait_recv()

    def await_first(i):
        pl.when(c == 0)(functools.partial(await_partner, i))
        pl.when(c == 1)(functools.partial(await_own, i))
        return i + n_own * (1 - c)

    def await_second(i):
        pl.when(c == 0)(functools.partial(await_own, i))
        pl.when(c == 1)(functools.partial(await_partner, i))
        return i + n_own * c

    def apply(s, b, start, n):
        start = b * rows + start
        at = span(start, n)
        gate_up(s, start, n)
        acc[y, at, :] = acc[y, at, :] + weighted(s, start, n, y)

    def all_rows(s):
        def step(b, carry):
            apply(s, b, 0, rows)
            return carry

        lax.fori_loop(0, 4, step, 0)

    def round_one(i, carry):
        all_rows(await_first(i))
        all_rows(await_second(i))
        return carry

    last = n_own - 1
    lax.fori_loop(0, last - 1, round_one, 0)
    all_rows(await_first(last - 1))

    tile = 2 * chunk
    kept = rows - late_rows
    pieces = [(0, chunk), (chunk, chunk), (tile, tile), (2 * tile, rows - 2 * tile)]
    n_first = len(pieces)
    whole = [(0, rows)]
    fine = [(0, rows - tile), (rows - tile, tile - 32), (rows - 32, 32)]

    x_pieces = {(DG, 0): pieces, (XN, 0): [(kept, late_rows), (0, kept)], (DG, 1): whole, (DG, 2): whole, (XN, 1): whole, (XN, 2): fine}
    y_pieces = (whole, whole, fine)
    x_places = {kind: n for n, kind in enumerate(x_pieces)}
    landing = {DG: 0, XN: 1}

    def sums(stage, b, start, n):
        at = span(b * rows + start, n)
        return acc.at[y, at] if stage == 0 else acc.at[oy, at, pl.ds((stage - 1) * group, group)]

    def landed(buffer, slot, stage, start, n):
        at = span(start, n)
        return buffer.at[slot, at] if stage == 0 else buffer.at[slot, at, pl.ds((stage - 1) * group, group)]

    def send_x(b, stage, k):
        start, n = x_pieces[b, stage][k]
        slot = landing[b] + (2 if stage else 0)
        sem = x_places[b, stage]
        return remote(sums(stage, b, start, n), landed(rx, slot, stage, start, n), cx_s.at[sem, k], cx_r.at[sem, k], x_dev)

    def send_y(stage, k):
        start, n = y_pieces[stage][k]
        return remote(sums(stage, YN, start, n), landed(ry, 1 if stage else 0, stage, start, n), cy_s.at[stage, k], cy_r.at[stage, k], y_dev)

    late_o = remote(o_out, o_in, o_s, o_r, x_dev)

    def add_rows(part, b, start, n, got, col=0, n_col=half_w):
        at, cols = span(b * rows + start, n), pl.ds(col, n_col)
        acc[part, at, cols] = acc[part, at, cols] + got[:, cols]

    def finish(part, start, n, col=0, n_col=half_w):
        at, cols = span(start, n), pl.ds(col, n_col)
        first = acc[part, at, cols] + weighted(last, start, n, part, col, n_col)
        acc[part, at, cols] = first + weighted(n_own + last, start, n, part, col, n_col)

    before_last = await_second(last - 1)
    apply(before_last, XN, 0, rows)
    early = await_first(last)
    apply(early, XN, 0, rows)
    send_x(XN, 0, 0).start()
    apply(before_last, DG, 0, rows)
    apply(early, DG, 0, rows)
    late = await_second(last)
    pl.when(c == 1)(send_down)
    for k, (start, n) in enumerate(pieces):
        apply(late, DG, start, n)
        send_x(DG, 0, k).start()
    gate_up(late, XN * rows + kept, late_rows)
    o_out[...] = expert_rows(late, XN * rows + kept, late_rows, y)
    late_o.start()
    apply(late, XN, 0, kept)
    send_x(XN, 0, 1).start()
    for s in (before_last, early, late):
        for b in (YN, OWN):
            apply(s, b, 0, rows)

    def arrive_d(g, i):
        arrived_d(g, i).wait_recv()
        fwd_d(g, i).start()

    def round_two(i, carry, g=0):
        arrive_d(g, i)
        down(i, g)
        fwd_d(g, i).wait_recv()
        down(n_own + i, g)
        return carry

    def close_two(g, b):
        finish(oy, b * rows, rows, g * group, group)

    lax.fori_loop(0, n_own - 1, functools.partial(round_two, g=0), 0)
    arrive_d(0, last)
    fwd_d(0, last).wait_recv()

    def add_x(part, b, stage, k):
        start, n = x_pieces[b, stage][k]
        send_x(b, stage, k).wait_recv()
        slot = landing[b] + (2 if stage else 0)
        add_rows(part, YN if b == DG else OWN, start, n, rx.at[slot, span(start, n)], *columns(stage))

    def add_y(part, stage, k):
        start, n = y_pieces[stage][k]
        send_y(stage, k).wait_recv()
        add_rows(part, OWN, start, n, ry.at[1 if stage else 0, span(start, n)], *columns(stage))

    def columns(stage):
        return (0, half_w) if stage == 0 else ((stage - 1) * group, group)

    close_two(0, DG)
    send_x(DG, 1, 0).start()

    def others(b, carry):
        close_two(0, b)
        return carry

    lax.fori_loop(OWN, DG, others, 0)
    for k in range(n_first):
        add_x(y, DG, 0, k)
    send_y(0, 0).start()

    lax.fori_loop(0, n_own - 1, functools.partial(round_two, g=1), 0)
    arrive_d(1, last)
    fwd_d(1, last).wait_recv()
    close_two(1, DG)
    send_x(DG, 2, 0).start()
    send_x(XN, 1, 0).start()
    close_two(1, XN)
    for k in range(len(fine)):
        send_x(XN, 2, k).start()
    close_two(1, YN)
    add_x(oy, DG, 1, 0)
    send_y(1, 0).start()
    close_two(1, OWN)
    add_x(oy, DG, 2, 0)
    for k in range(len(fine)):
        send_y(2, k).start()
    add_x(y, XN, 0, 0)
    add_x(y, XN, 0, 1)
    late_o.wait_recv()
    at_late = span(kept, late_rows)
    acc[y, at_late, :] = acc[y, at_late, :] + scaled(gcol_x[at_late, :], late, o_in[...])
    add_y(oy, 0, 0)
    add_y(y, 1, 0)
    add_x(oy, XN, 1, 0)

    def result(k):
        start, n = fine[k]
        return pltpu.make_async_copy(tok.at[span(start, n)], out_hbm.at[span(start, n)], out_sem.at[k])

    for k, (start, n) in enumerate(fine):
        at = span(start, n)
        add_y(y, 2, k)
        add_x(oy, XN, 2, k)
        for part in range(2):
            cols = pl.ds(part * half_w, half_w)
            tok[at, cols] = (tok[at, cols].astype(jnp.float32) + acc[part, at, :]).astype(tok.dtype)
        result(k).start()

    def drain_w(i, carry):
        for m in range(3):
            partner_own(m, i).wait_send()
        for m in range(2):
            send_w(m, i).wait_send()
            partner_fwd(m, i).wait_send()
        for g in range(2):
            send_d(g, i).wait_send()
            fwd_d(g, i).wait_send()
        return carry

    lax.fori_loop(0, n_own, drain_w, 0)
    for (b, stage), some in x_pieces.items():
        for k in range(len(some)):
            send_x(b, stage, k).wait_send()
    for stage, some in enumerate(y_pieces):
        for k in range(len(some)):
            send_y(stage, k).wait_send()
    pl.when(c == 0)(tok_y.wait_send)
    for cp in (late_o, tok_x, tok_d, g_x, g_y, g_d):
        cp.wait_send()
    for k in range(len(fine)):
        result(k).wait()


def solution(mesh):
    ep_size = mesh.shape["ep"]
    row_spec = P(("rep", "ep", "fsdp"), None)

    def device_step(tokens, expert_idx, gates, w_gate, w_up, w_down):
        rows, top_k = expert_idx.shape
        n_local, half_w, ffn = w_gate.shape
        width = tokens.shape[1]
        n_own = n_local // 2
        num_experts = n_local * ep_size
        capacity = (2 * rows * top_k + num_experts - 1) // num_experts
        chunk, late_rows = 64, 128
        dma = pltpu.SemaphoreType.DMA
        hbm = pl.BlockSpec(memory_space=pl.ANY)
        return pl.pallas_call(
            functools.partial(moe_kernel, num_experts, capacity, chunk, late_rows),
            out_shape=jax.ShapeDtypeStruct((rows, width), jnp.bfloat16),
            in_specs=[hbm] * 6,
            out_specs=hbm,
            scratch_shapes=[
                pltpu.VMEM((top_k, rows), jnp.int32),
                pltpu.VMEM((top_k, rows), jnp.float32),
                pltpu.VMEM((4 * rows, width), jnp.bfloat16),
                pltpu.VMEM((3, n_local, 2, half_w, ffn), jnp.bfloat16),
                pltpu.VMEM((2, 4 * rows, half_w), jnp.float32),
                pltpu.VMEM((n_local, 4 * rows, ffn), jnp.bfloat16),
                pltpu.VMEM((num_experts, rows), jnp.float32),
                pltpu.VMEM((4 * n_local, rows), jnp.float32),
                pltpu.VMEM((4 * rows, 128), jnp.float32),
                pltpu.VMEM((rows, 128), jnp.float32),
                pltpu.VMEM((4, rows, half_w), jnp.float32),
                pltpu.VMEM((2, rows, half_w), jnp.float32),
                pltpu.VMEM((late_rows, half_w), jnp.bfloat16),
                pltpu.VMEM((late_rows, half_w), jnp.bfloat16),
                pltpu.SemaphoreType.REGULAR,
                dma((2,)), dma((3,)), dma, dma((3,)), dma((3,)), dma((3,)), dma((3,)),
                dma((3, n_own)), dma((3, n_own)), dma((3, n_own)),
                dma((3, n_own)), dma((3, n_own)), dma((2, n_own)), dma((2, n_own)),
                dma((2, n_own)), dma((2, n_own)), dma((2, n_own)), dma((2, n_own)),
                dma((6, 4)), dma((6, 4)), dma((3, 3)), dma((3, 3)), dma, dma,
            ],
            compiler_params=pltpu.CompilerParams(collective_id=0, has_side_effects=True, vmem_limit_bytes=67_043_328),
        )(tokens, expert_idx.T, gates.T, w_gate, w_up, w_down)

    return jax.shard_map(device_step, mesh=mesh, in_specs=(row_spec, row_spec, row_spec, P("ep", "fsdp", None), P("ep", "fsdp", None), P("ep", None, "fsdp")), out_specs=row_spec, check_vma=False)
```

```python
import functools

import jax
import jax.numpy as jnp
from jax import lax
from jax.experimental import pallas as pl
from jax.experimental.pallas import tpu as pltpu
from jax.sharding import PartitionSpec as P

MESH = pl.DeviceIdType.MESH
OWN, XN, YN, DG = 0, 1, 2, 3


def moe_kernel(num_experts, capacity, chunk, late_rows, tokens_hbm, idx_hbm, gates_hbm, wg_hbm, wu_hbm, wd_hbm, out_hbm,
               idx_ref, gates_ref, tok, w, acc, hid, gt_send, gt_recv, gcol, gcol_x, rx, ry, o_out, o_in, go_sem,
               small_sem, out_sem, loc_tok_sem, tok_send, tok_recv, g_send, g_recv_sem, loc_sem, ys_sem, yr_sem,
               po_s, po_r, pf_s, pf_r, ds_sem, dr_sem, df_s, df_r, cx_s, cx_r, cy_s, cy_r, o_s, o_r):
    rows, width = out_hbm.shape
    n_local = wg_hbm.shape[0]
    n_own = n_local // 2
    half_w = width // 2
    group = half_w // 2
    n_chunk = rows // chunk
    ep = lax.axis_index("ep")
    y = lax.axis_index("fsdp")
    c = lax.rem(ep, 2)
    x = ep // 2
    oy = 1 - y
    x_dev = {"ep": lax.rem(ep + 2, 4), "fsdp": y}
    y_dev = {"ep": ep, "fsdp": oy}
    p_dev = {"ep": ep + 1 - 2 * c, "fsdp": y}
    w_hbm = (wg_hbm, wu_hbm, wd_hbm)

    def remote(src, dst, s, r, dev):
        return pltpu.make_async_remote_copy(src_ref=src, dst_ref=dst, send_sem=s, recv_sem=r, device_id=dev, device_id_type=MESH)

    def span(start, n):
        return pl.ds(pl.multiple_of(start, 16), n)

    def block(b):
        return tok.at[pl.ds(b * rows, rows)]

    idx_in = pltpu.make_async_copy(idx_hbm, idx_ref, small_sem.at[0])
    gates_in = pltpu.make_async_copy(gates_hbm, gates_ref, small_sem.at[1])
    idx_in.start()
    gates_in.start()
    barrier = pltpu.get_barrier_semaphore()
    for dev in (y_dev, x_dev, p_dev):
        pl.semaphore_signal(barrier, inc=1, device_id=dev, device_id_type=MESH)
    pl.semaphore_wait(barrier, 3)

    tok_y = remote(tokens_hbm, block(YN), tok_send.at[0], tok_recv.at[0], y_dev)
    tok_x = remote(tokens_hbm, block(XN), tok_send.at[1], tok_recv.at[1], x_dev)
    tok_d = remote(block(YN), block(DG), tok_send.at[2], tok_recv.at[2], x_dev)
    tok_l = pltpu.make_async_copy(tokens_hbm, block(OWN), loc_tok_sem)
    tok_x.start()
    tok_l.start()

    @pl.when(c == 1)
    def _():
        tok_y.start()

    row = lax.broadcasted_iota(jnp.int32, (num_experts, 1), 0)
    dest, slot = row // n_local, lax.rem(row, n_local)
    dx, dy = lax.rem(dest, 2), dest // 2
    ex = x + dx - 2 * x * dx
    ey = y + dy - 2 * y * dy
    sc = slot // n_own
    ec = c + sc - 2 * c * sc
    expert = (2 * ex + ec) * n_local + ey * n_own + lax.rem(slot, n_own)
    idx_in.wait()
    gates_in.wait()
    dense = jnp.zeros((num_experts, rows), jnp.float32)
    chosen = jnp.zeros((num_experts, rows), jnp.float32)
    for j in range(idx_ref.shape[0]):
        hit = idx_ref[j:j + 1, :] == expert
        dense = jnp.where(hit, gates_ref[j:j + 1, :], dense)
        chosen = jnp.where(hit, 1.0, chosen)
    before = lax.broadcasted_iota(jnp.int32, (rows, rows), 0) < lax.broadcasted_iota(jnp.int32, (rows, rows), 1)
    taken = jnp.dot(chosen.astype(jnp.bfloat16), before.astype(jnp.bfloat16), preferred_element_type=jnp.float32)
    dense = jnp.where(taken < float(capacity), dense, 0.0)
    gt_send[...] = dense
    g_x = remote(gt_send.at[pl.ds(XN * n_local, n_local)], gt_recv.at[pl.ds(0, n_local)], g_send.at[0], g_recv_sem.at[0], x_dev)
    g_y = remote(gt_send.at[pl.ds(YN * n_local, 2 * n_local)], gt_recv.at[pl.ds(n_local, 2 * n_local)], g_send.at[1], g_recv_sem.at[1], y_dev)
    g_d = remote(gt_recv.at[pl.ds(2 * n_local, n_local)], gt_recv.at[pl.ds(3 * n_local, n_local)], g_send.at[2], g_recv_sem.at[2], x_dev)


    g_x.start()

    def local_w(m, i):
        return pltpu.make_async_copy(w_hbm[m].at[y * n_own + i], w.at[m, i, y], loc_sem.at[m, i])

    def send_w(m, i):
        return remote(w_hbm[m].at[oy * n_own + i], w.at[m, i, y], ys_sem.at[m, i], yr_sem.at[m, i], y_dev)

    def arrived_w(m, i):
        return remote(w_hbm[m].at[oy * n_own + i], w.at[m, i, oy], ys_sem.at[m, i], yr_sem.at[m, i], y_dev)

    def partner_own(m, i):
        return remote(w_hbm[m].at[y * n_own + i], w.at[m, n_own + i, y], po_s.at[m, i], po_r.at[m, i], p_dev)

    def partner_fwd(m, i):
        return remote(w.at[m, i, oy], w.at[m, n_own + i, oy], pf_s.at[m, i], pf_r.at[m, i], p_dev)

    def down_half(slot, part, g):
        return w.at[2, slot, part, :, pl.ds(g * group, group)]

    def send_d(g, i):
        return remote(wd_hbm.at[oy * n_own + i, :, pl.ds(g * group, group)], down_half(i, y, g), ds_sem.at[g, i], dr_sem.at[g, i], y_dev)

    def arrived_d(g, i):
        return remote(wd_hbm.at[oy * n_own + i, :, pl.ds(g * group, group)], down_half(i, oy, g), ds_sem.at[g, i], dr_sem.at[g, i], y_dev)

    def fwd_d(g, i):
        return remote(down_half(i, oy, g), down_half(n_own + i, oy, g), df_s.at[g, i], df_r.at[g, i], p_dev)

    def send_gate_up():
        for i in range(n_own):
            for m in range(2):
                send_w(m, i).start()

    @pl.when(c == 1)
    def _():
        g_y.start()
        send_gate_up()

    def send_down():
        for g in range(2):
            for i in range(n_own):
                send_d(g, i).start()

    for i in range(n_own):
        for m in range(3):
            local_w(m, i).start()
            partner_own(m, i).start()

    def clear(k, carry):
        for part in range(2):
            acc[part, span(k * chunk, chunk), :] = jnp.zeros((chunk, half_w), jnp.float32)
        return carry

    lax.fori_loop(0, 4 * n_chunk, clear, 0)

    @pl.when(c == 1)
    def _():
        tok_y.wait_send()
        pl.semaphore_signal(go_sem, inc=1, device_id=p_dev, device_id_type=MESH)

    @pl.when(c == 0)
    def _():
        pl.semaphore_wait(go_sem, 1)
        tok_y.start()
        g_y.start()
        send_gate_up()
        send_down()

    def columns_of(g):
        return jnp.concatenate([g, jnp.zeros((128 - n_local, rows), jnp.float32)], axis=0).T

    def column_gates(b, g):
        gcol[pl.ds(b * rows, rows), :] = columns_of(g)

    column_gates(OWN, gt_send[0:n_local, :])
    gcol_x[...] = columns_of(gt_send[pl.ds(XN * n_local, n_local), :])
    tok_y.wait_recv()
    tok_d.start()
    g_y.wait_recv()
    g_d.start()
    for k, (b, cp) in enumerate(((XN, g_x), (YN, None), (None, None), (DG, g_d))):
        if cp is not None:
            cp.wait_recv()
        if b is not None:
            column_gates(b, gt_recv[k * n_local:(k + 1) * n_local, :])

    tok_l.wait()
    tok_x.wait_recv()
    tok_d.wait_recv()

    lane = lax.broadcasted_iota(jnp.int32, (1, 128), 1)

    def gate_up(s, start, n):
        at = span(start, n)
        r = tok[at, :]
        a = jnp.dot(r, w[0, s].reshape(width, w.shape[-1]), preferred_element_type=jnp.float32)
        u = jnp.dot(r, w[1, s].reshape(width, w.shape[-1]), preferred_element_type=jnp.float32)
        hid[s, at, :] = (a * jax.nn.sigmoid(a) * u).astype(jnp.bfloat16)

    def expert_rows(s, start, n, part, col=0, n_col=half_w):
        return jnp.dot(hid[s, span(start, n), :], w[2, s, part, :, pl.ds(col, n_col)], preferred_element_type=jnp.float32).astype(jnp.bfloat16)

    def scaled(gates, s, o):
        g = jnp.sum(jnp.where(lane == s, gates, 0.0), axis=1, keepdims=True)
        return jnp.where(g != 0.0, g * o.astype(jnp.float32), 0.0)

    def weighted(s, start, n, part, col=0, n_col=half_w):
        return scaled(gcol[span(start, n), :], s, expert_rows(s, start, n, part, col, n_col))

    def down(s, g):
        cols = pl.ds(g * group, group)
        step_rows = rows // 2

        def step(k, carry):
            at = span(k * step_rows, step_rows)
            acc[oy, at, cols] = acc[oy, at, cols] + weighted(s, k * step_rows, step_rows, oy, g * group, group)
            return carry

        lax.fori_loop(0, 8, step, 0)

    def arrive(m, i):
        arrived_w(m, i).wait_recv()
        partner_fwd(m, i).start()

    def await_own(i):
        for m in range(2):
            arrive(m, i)
        for m in range(3):
            local_w(m, i).wait()

    def await_partner(i):
        for m in range(3):
            partner_own(m, i).wait_recv()
        for m in range(2):
            partner_fwd(m, i).wait_recv()

    def await_first(i):
        pl.when(c == 0)(functools.partial(await_partner, i))
        pl.when(c == 1)(functools.partial(await_own, i))
        return i + n_own * (1 - c)

    def await_second(i):
        pl.when(c == 0)(functools.partial(await_own, i))
        pl.when(c == 1)(functools.partial(await_partner, i))
        return i + n_own * c

    def apply(s, b, start, n):
        size = min(n, rows // 2) if n % (rows // 2) == 0 else n if n < rows // 2 else 2 * chunk

        def step(k, carry):
            first = b * rows + start + k * size
            at = span(first, size)
            gate_up(s, first, size)
            acc[y, at, :] = acc[y, at, :] + weighted(s, first, size, y)
            return carry

        lax.fori_loop(0, n // size, step, 0)

    def all_rows(s):
        def step(b, carry):
            apply(s, b, 0, rows)
            return carry

        lax.fori_loop(0, 4, step, 0)

    def round_one(i, carry):
        all_rows(await_first(i))
        all_rows(await_second(i))
        return carry

    last = n_own - 1
    lax.fori_loop(0, last - 1, round_one, 0)
    all_rows(await_first(last - 1))

    tile = 2 * chunk
    kept = rows - late_rows
    pieces = [(0, chunk), (chunk, chunk), (tile, tile), (2 * tile, rows - 2 * tile)]
    n_first = len(pieces)
    whole = [(0, rows)]
    fine = [(0, rows - tile), (rows - tile, tile - 32), (rows - 32, 32)]

    x_pieces = {(DG, 0): pieces, (XN, 0): [(kept, late_rows), (0, kept)], (DG, 1): whole, (DG, 2): whole, (XN, 1): whole, (XN, 2): fine}
    y_pieces = (whole, whole, fine)
    x_places = {kind: n for n, kind in enumerate(x_pieces)}
    landing = {DG: 0, XN: 1}

    def sums(stage, b, start, n):
        at = span(b * rows + start, n)
        return acc.at[y, at] if stage == 0 else acc.at[oy, at, pl.ds((stage - 1) * group, group)]

    def landed(buffer, slot, stage, start, n):
        at = span(start, n)
        return buffer.at[slot, at] if stage == 0 else buffer.at[slot, at, pl.ds((stage - 1) * group, group)]

    def send_x(b, stage, k):
        start, n = x_pieces[b, stage][k]
        slot = landing[b] + (2 if stage else 0)
        sem = x_places[b, stage]
        return remote(sums(stage, b, start, n), landed(rx, slot, stage, start, n), cx_s.at[sem, k], cx_r.at[sem, k], x_dev)

    def send_y(stage, k):
        start, n = y_pieces[stage][k]
        return remote(sums(stage, YN, start, n), landed(ry, 1 if stage else 0, stage, start, n), cy_s.at[stage, k], cy_r.at[stage, k], y_dev)

    late_o = remote(o_out, o_in, o_s, o_r, x_dev)

    def add_rows(part, b, start, n, got, col=0, n_col=half_w):
        at, cols = span(b * rows + start, n), pl.ds(col, n_col)
        acc[part, at, cols] = acc[part, at, cols] + got[:, cols]

    def finish(part, start, n, col=0, n_col=half_w):
        at, cols = span(start, n), pl.ds(col, n_col)
        first = acc[part, at, cols] + weighted(last, start, n, part, col, n_col)
        acc[part, at, cols] = first + weighted(n_own + last, start, n, part, col, n_col)

    before_last = await_second(last - 1)
    apply(before_last, XN, 0, rows)
    early = await_first(last)
    apply(early, XN, 0, rows)
    send_x(XN, 0, 0).start()
    apply(before_last, DG, 0, rows)
    apply(early, DG, 0, rows)
    late = await_second(last)
    pl.when(c == 1)(send_down)
    for k, (start, n) in enumerate(pieces):
        apply(late, DG, start, n)
        send_x(DG, 0, k).start()
    gate_up(late, XN * rows + kept, late_rows)
    o_out[...] = expert_rows(late, XN * rows + kept, late_rows, y)
    late_o.start()
    apply(late, XN, 0, kept)
    send_x(XN, 0, 1).start()
    for s in (before_last, early, late):
        for b in (YN, OWN):
            apply(s, b, 0, rows)

    def arrive_d(g, i):
        arrived_d(g, i).wait_recv()
        fwd_d(g, i).start()

    def round_two(i, carry, g=0):
        arrive_d(g, i)
        down(i, g)
        fwd_d(g, i).wait_recv()
        down(n_own + i, g)
        return carry

    def close_two(g, b):
        def step(k, carry):
            finish(oy, b * rows + k * (rows // 2), rows // 2, g * group, group)
            return carry

        lax.fori_loop(0, 2, step, 0)

    lax.fori_loop(0, n_own - 1, functools.partial(round_two, g=0), 0)
    arrive_d(0, last)
    fwd_d(0, last).wait_recv()

    def add_x(part, b, stage, k):
        start, n = x_pieces[b, stage][k]
        send_x(b, stage, k).wait_recv()
        slot = landing[b] + (2 if stage else 0)
        add_rows(part, YN if b == DG else OWN, start, n, rx.at[slot, span(start, n)], *columns(stage))

    def add_y(part, stage, k):
        start, n = y_pieces[stage][k]
        send_y(stage, k).wait_recv()
        add_rows(part, OWN, start, n, ry.at[1 if stage else 0, span(start, n)], *columns(stage))

    def columns(stage):
        return (0, half_w) if stage == 0 else ((stage - 1) * group, group)

    close_two(0, DG)
    send_x(DG, 1, 0).start()

    def others(b, carry):
        close_two(0, b)
        return carry

    lax.fori_loop(OWN, DG, others, 0)
    for k in range(n_first):
        add_x(y, DG, 0, k)
    send_y(0, 0).start()

    lax.fori_loop(0, n_own - 1, functools.partial(round_two, g=1), 0)
    arrive_d(1, last)
    fwd_d(1, last).wait_recv()
    close_two(1, DG)
    send_x(DG, 2, 0).start()
    send_x(XN, 1, 0).start()
    close_two(1, XN)
    for k in range(len(fine)):
        send_x(XN, 2, k).start()
    close_two(1, YN)
    add_x(oy, DG, 1, 0)
    send_y(1, 0).start()
    close_two(1, OWN)
    add_x(oy, DG, 2, 0)
    for k in range(len(fine)):
        send_y(2, k).start()
    add_x(y, XN, 0, 0)
    add_x(y, XN, 0, 1)
    late_o.wait_recv()
    at_late = span(kept, late_rows)
    acc[y, at_late, :] = acc[y, at_late, :] + scaled(gcol_x[at_late, :], late, o_in[...])
    add_y(oy, 0, 0)
    add_y(y, 1, 0)
    add_x(oy, XN, 1, 0)

    def result(k):
        start, n = fine[k]
        return pltpu.make_async_copy(tok.at[span(start, n)], out_hbm.at[span(start, n)], out_sem.at[k])

    for k, (start, n) in enumerate(fine):
        at = span(start, n)
        add_y(y, 2, k)
        add_x(oy, XN, 2, k)
        cut = n // 2 if n > tile else n
        for a in range(start, start + n, cut):
            rows_at = span(a, cut)
            for part in range(2):
                cols = pl.ds(part * half_w, half_w)
                tok[rows_at, cols] = (tok[rows_at, cols].astype(jnp.float32) + acc[part, rows_at, :]).astype(tok.dtype)
        result(k).start()

    def drain_w(i, carry):
        for m in range(3):
            partner_own(m, i).wait_send()
        for m in range(2):
            send_w(m, i).wait_send()
            partner_fwd(m, i).wait_send()
        for g in range(2):
            send_d(g, i).wait_send()
            fwd_d(g, i).wait_send()
        return carry

    lax.fori_loop(0, n_own, drain_w, 0)
    for (b, stage), some in x_pieces.items():
        for k in range(len(some)):
            send_x(b, stage, k).wait_send()
    for stage, some in enumerate(y_pieces):
        for k in range(len(some)):
            send_y(stage, k).wait_send()
    pl.when(c == 0)(tok_y.wait_send)
    for cp in (late_o, tok_x, tok_d, g_x, g_y, g_d):
        cp.wait_send()
    for k in range(len(fine)):
        result(k).wait()


def solution(mesh):
    ep_size = mesh.shape["ep"]
    row_spec = P(("rep", "ep", "fsdp"), None)

    def device_step(tokens, expert_idx, gates, w_gate, w_up, w_down):
        rows, top_k = expert_idx.shape
        n_local, half_w, ffn = w_gate.shape
        width = tokens.shape[1]
        n_own = n_local // 2
        num_experts = n_local * ep_size
        capacity = (2 * rows * top_k + num_experts - 1) // num_experts
        chunk, late_rows = 64, 128
        dma = pltpu.SemaphoreType.DMA
        hbm = pl.BlockSpec(memory_space=pl.ANY)
        return pl.pallas_call(
            functools.partial(moe_kernel, num_experts, capacity, chunk, late_rows),
            out_shape=pltpu.VMEM((rows, width), jnp.bfloat16),
            in_specs=[hbm] * 6,
            out_specs=hbm,
            scratch_shapes=[
                pltpu.VMEM((top_k, rows), jnp.int32),
                pltpu.VMEM((top_k, rows), jnp.float32),
                pltpu.VMEM((4 * rows, width), jnp.bfloat16),
                pltpu.VMEM((3, n_local, 2, half_w, ffn), jnp.bfloat16),
                pltpu.VMEM((2, 4 * rows, half_w), jnp.float32),
                pltpu.VMEM((n_local, 4 * rows, ffn), jnp.bfloat16),
                pltpu.VMEM((num_experts, rows), jnp.float32),
                pltpu.VMEM((4 * n_local, rows), jnp.float32),
                pltpu.VMEM((4 * rows, 128), jnp.float32),
                pltpu.VMEM((rows, 128), jnp.float32),
                pltpu.VMEM((4, rows, half_w), jnp.float32),
                pltpu.VMEM((2, rows, half_w), jnp.float32),
                pltpu.VMEM((late_rows, half_w), jnp.bfloat16),
                pltpu.VMEM((late_rows, half_w), jnp.bfloat16),
                pltpu.SemaphoreType.REGULAR,
                dma((2,)), dma((3,)), dma, dma((3,)), dma((3,)), dma((3,)), dma((3,)),
                dma((3, n_own)), dma((3, n_own)), dma((3, n_own)),
                dma((3, n_own)), dma((3, n_own)), dma((2, n_own)), dma((2, n_own)),
                dma((2, n_own)), dma((2, n_own)), dma((2, n_own)), dma((2, n_own)),
                dma((6, 4)), dma((6, 4)), dma((3, 3)), dma((3, 3)), dma, dma,
            ],
            compiler_params=pltpu.CompilerParams(collective_id=0, has_side_effects=True, vmem_limit_bytes=64_900_000),
        )(tokens, expert_idx.T, gates.T, w_gate, w_up, w_down)

    return jax.shard_map(device_step, mesh=mesh, in_specs=(row_spec, row_spec, row_spec, P("ep", "fsdp", None), P("ep", "fsdp", None), P("ep", None, "fsdp")), out_specs=row_spec, check_vma=False)
```

```python
import functools

import jax
import jax.numpy as jnp
from jax import lax
from jax.experimental import pallas as pl
from jax.experimental.pallas import tpu as pltpu
from jax.sharding import PartitionSpec as P

MESH = pl.DeviceIdType.MESH
OWN, XN, YN, DG = 0, 1, 2, 3


def moe_kernel(num_experts, capacity, chunk, late_rows, tokens_hbm, idx_hbm, gates_hbm, wg_hbm, wu_hbm, wd_hbm, out_hbm,
               idx_ref, gates_ref, tok, w, acc, hid, gt_send, gt_recv, gcol, gcol_x, rx, ry, o_out, o_in, go_sem,
               small_sem, out_sem, loc_tok_sem, tok_send, tok_recv, g_send, g_recv_sem, loc_sem, ys_sem, yr_sem,
               po_s, po_r, pf_s, pf_r, ds_sem, dr_sem, df_s, df_r, cx_s, cx_r, cy_s, cy_r, o_s, o_r):
    rows, width = out_hbm.shape
    n_local = wg_hbm.shape[0]
    n_own = n_local // 2
    half_w = width // 2
    group = half_w // 2
    n_chunk = rows // chunk
    ep = lax.axis_index("ep")
    y = lax.axis_index("fsdp")
    c = lax.rem(ep, 2)
    x = ep // 2
    oy = 1 - y
    x_dev = {"ep": lax.rem(ep + 2, 4), "fsdp": y}
    y_dev = {"ep": ep, "fsdp": oy}
    p_dev = {"ep": ep + 1 - 2 * c, "fsdp": y}
    w_hbm = (wg_hbm, wu_hbm, wd_hbm)

    def remote(src, dst, s, r, dev):
        return pltpu.make_async_remote_copy(src_ref=src, dst_ref=dst, send_sem=s, recv_sem=r, device_id=dev, device_id_type=MESH)

    def span(start, n):
        return pl.ds(pl.multiple_of(start, 16), n)

    def block(b):
        return tok.at[pl.ds(b * rows, rows)]

    idx_in = pltpu.make_async_copy(idx_hbm, idx_ref, small_sem.at[0])
    gates_in = pltpu.make_async_copy(gates_hbm, gates_ref, small_sem.at[1])
    idx_in.start()
    gates_in.start()
    barrier = pltpu.get_barrier_semaphore()
    for dev in (y_dev, x_dev, p_dev):
        pl.semaphore_signal(barrier, inc=1, device_id=dev, device_id_type=MESH)
    pl.semaphore_wait(barrier, 3)

    tok_y = remote(tokens_hbm, block(YN), tok_send.at[0], tok_recv.at[0], y_dev)
    tok_x = remote(tokens_hbm, block(XN), tok_send.at[1], tok_recv.at[1], x_dev)
    tok_d = remote(block(YN), block(DG), tok_send.at[2], tok_recv.at[2], x_dev)
    tok_l = pltpu.make_async_copy(tokens_hbm, block(OWN), loc_tok_sem)
    tok_x.start()
    tok_l.start()

    @pl.when(c == 1)
    def _():
        tok_y.start()

    row = lax.broadcasted_iota(jnp.int32, (num_experts, 1), 0)
    dest, slot = row // n_local, lax.rem(row, n_local)
    dx, dy = lax.rem(dest, 2), dest // 2
    ex = x + dx - 2 * x * dx
    ey = y + dy - 2 * y * dy
    sc = slot // n_own
    ec = c + sc - 2 * c * sc
    expert = (2 * ex + ec) * n_local + ey * n_own + lax.rem(slot, n_own)
    idx_in.wait()
    gates_in.wait()
    dense = jnp.zeros((num_experts, rows), jnp.float32)
    chosen = jnp.zeros((num_experts, rows), jnp.float32)
    for j in range(idx_ref.shape[0]):
        hit = idx_ref[j:j + 1, :] == expert
        dense = jnp.where(hit, gates_ref[j:j + 1, :], dense)
        chosen = jnp.where(hit, 1.0, chosen)
    before = lax.broadcasted_iota(jnp.int32, (rows, rows), 0) < lax.broadcasted_iota(jnp.int32, (rows, rows), 1)
    taken = jnp.dot(chosen.astype(jnp.bfloat16), before.astype(jnp.bfloat16), preferred_element_type=jnp.float32)
    dense = jnp.where(taken < float(capacity), dense, 0.0)
    gt_send[...] = dense
    g_x = remote(gt_send.at[pl.ds(XN * n_local, n_local)], gt_recv.at[pl.ds(0, n_local)], g_send.at[0], g_recv_sem.at[0], x_dev)
    g_y = remote(gt_send.at[pl.ds(YN * n_local, 2 * n_local)], gt_recv.at[pl.ds(n_local, 2 * n_local)], g_send.at[1], g_recv_sem.at[1], y_dev)
    g_d = remote(gt_recv.at[pl.ds(2 * n_local, n_local)], gt_recv.at[pl.ds(3 * n_local, n_local)], g_send.at[2], g_recv_sem.at[2], x_dev)


    g_x.start()

    def local_w(m, i):
        return pltpu.make_async_copy(w_hbm[m].at[y * n_own + i], w.at[m, i, y], loc_sem.at[m, i])

    def send_w(m, i):
        return remote(w_hbm[m].at[oy * n_own + i], w.at[m, i, y], ys_sem.at[m, i], yr_sem.at[m, i], y_dev)

    def arrived_w(m, i):
        return remote(w_hbm[m].at[oy * n_own + i], w.at[m, i, oy], ys_sem.at[m, i], yr_sem.at[m, i], y_dev)

    def partner_own(m, i):
        return remote(w_hbm[m].at[y * n_own + i], w.at[m, n_own + i, y], po_s.at[m, i], po_r.at[m, i], p_dev)

    def partner_fwd(m, i):
        return remote(w.at[m, i, oy], w.at[m, n_own + i, oy], pf_s.at[m, i], pf_r.at[m, i], p_dev)

    def down_half(slot, part, g):
        return w.at[2, slot, part, :, pl.ds(g * group, group)]

    def send_d(g, i):
        return remote(wd_hbm.at[oy * n_own + i, :, pl.ds(g * group, group)], down_half(i, y, g), ds_sem.at[g, i], dr_sem.at[g, i], y_dev)

    def arrived_d(g, i):
        return remote(wd_hbm.at[oy * n_own + i, :, pl.ds(g * group, group)], down_half(i, oy, g), ds_sem.at[g, i], dr_sem.at[g, i], y_dev)

    def fwd_d(g, i):
        return remote(down_half(i, oy, g), down_half(n_own + i, oy, g), df_s.at[g, i], df_r.at[g, i], p_dev)

    def send_gate_up():
        for i in range(n_own):
            for m in range(2):
                send_w(m, i).start()

    @pl.when(c == 1)
    def _():
        g_y.start()
        send_gate_up()

    def send_down():
        for g in range(2):
            for i in range(n_own):
                send_d(g, i).start()

    for i in range(n_own):
        for m in range(3):
            local_w(m, i).start()
            partner_own(m, i).start()

    def clear(k, carry):
        for part in range(2):
            acc[part, span(k * chunk, chunk), :] = jnp.zeros((chunk, half_w), jnp.float32)
        return carry

    lax.fori_loop(0, 4 * n_chunk, clear, 0)

    @pl.when(c == 1)
    def _():
        tok_y.wait_send()
        pl.semaphore_signal(go_sem, inc=1, device_id=p_dev, device_id_type=MESH)

    @pl.when(c == 0)
    def _():
        pl.semaphore_wait(go_sem, 1)
        tok_y.start()
        g_y.start()
        send_gate_up()
        send_down()

    def columns_of(g):
        return jnp.concatenate([g, jnp.zeros((128 - n_local, rows), jnp.float32)], axis=0).T

    def column_gates(b, g):
        gcol[pl.ds(b * rows, rows), :] = columns_of(g)

    column_gates(OWN, gt_send[0:n_local, :])
    gcol_x[...] = columns_of(gt_send[pl.ds(XN * n_local, n_local), :])
    tok_y.wait_recv()
    tok_d.start()
    g_y.wait_recv()
    g_d.start()
    for k, (b, cp) in enumerate(((XN, g_x), (YN, None), (None, None), (DG, g_d))):
        if cp is not None:
            cp.wait_recv()
        if b is not None:
            column_gates(b, gt_recv[k * n_local:(k + 1) * n_local, :])

    tok_l.wait()
    tok_x.wait_recv()
    tok_d.wait_recv()

    lane = lax.broadcasted_iota(jnp.int32, (1, 128), 1)

    def gate_up(s, start, n):
        at = span(start, n)
        r = tok[at, :]
        a = jnp.dot(r, w[0, s].reshape(width, w.shape[-1]), preferred_element_type=jnp.float32)
        u = jnp.dot(r, w[1, s].reshape(width, w.shape[-1]), preferred_element_type=jnp.float32)
        hid[s, at, :] = (a * jax.nn.sigmoid(a) * u).astype(jnp.bfloat16)

    def expert_rows(s, start, n, part, col=0, n_col=half_w):
        return jnp.dot(hid[s, span(start, n), :], w[2, s, part, :, pl.ds(col, n_col)], preferred_element_type=jnp.float32).astype(jnp.bfloat16)

    def scaled(gates, s, o):
        g = jnp.sum(jnp.where(lane == s, gates, 0.0), axis=1, keepdims=True)
        return jnp.where(g != 0.0, g * o.astype(jnp.float32), 0.0)

    def weighted(s, start, n, part, col=0, n_col=half_w):
        return scaled(gcol[span(start, n), :], s, expert_rows(s, start, n, part, col, n_col))

    def down(s, g):
        cols = pl.ds(g * group, group)
        step_rows = rows // 2

        def step(k, carry):
            at = span(k * step_rows, step_rows)
            acc[oy, at, cols] = acc[oy, at, cols] + weighted(s, k * step_rows, step_rows, oy, g * group, group)
            return carry

        lax.fori_loop(0, 8, step, 0)

    def arrive(m, i):
        arrived_w(m, i).wait_recv()
        partner_fwd(m, i).start()

    def await_own(i):
        for m in range(2):
            arrive(m, i)
        for m in range(3):
            local_w(m, i).wait()

    def await_partner(i):
        for m in range(3):
            partner_own(m, i).wait_recv()
        for m in range(2):
            partner_fwd(m, i).wait_recv()

    def await_first(i):
        pl.when(c == 0)(functools.partial(await_partner, i))
        pl.when(c == 1)(functools.partial(await_own, i))
        return i + n_own * (1 - c)

    def await_second(i):
        pl.when(c == 0)(functools.partial(await_own, i))
        pl.when(c == 1)(functools.partial(await_partner, i))
        return i + n_own * c

    def apply(s, b, start, n):
        size = n if n < rows // 2 else rows // 2 if n % (rows // 2) == 0 else n // 2

        def step(k, carry):
            first = b * rows + start + k * size
            at = span(first, size)
            gate_up(s, first, size)
            acc[y, at, :] = acc[y, at, :] + weighted(s, first, size, y)
            return carry

        lax.fori_loop(0, n // size, step, 0)

    def all_rows(s):
        def step(b, carry):
            apply(s, b, 0, rows)
            return carry

        lax.fori_loop(0, 4, step, 0)

    def round_one(i, carry):
        all_rows(await_first(i))
        all_rows(await_second(i))
        return carry

    last = n_own - 1
    lax.fori_loop(0, last - 1, round_one, 0)
    all_rows(await_first(last - 1))

    tile = 2 * chunk
    kept = rows - late_rows
    pieces = [(0, chunk), (chunk, chunk), (tile, tile), (2 * tile, rows - 2 * tile)]
    n_first = len(pieces)
    whole = [(0, rows)]
    fine = [(0, rows - tile), (rows - tile, tile - 32), (rows - 32, 32)]

    x_pieces = {(DG, 0): pieces, (XN, 0): [(kept, late_rows), (0, kept)], (DG, 1): whole, (DG, 2): whole, (XN, 1): whole, (XN, 2): fine}
    y_pieces = (whole, whole, fine)
    x_places = {kind: n for n, kind in enumerate(x_pieces)}
    landing = {DG: 0, XN: 1}

    def sums(stage, b, start, n):
        at = span(b * rows + start, n)
        return acc.at[y, at] if stage == 0 else acc.at[oy, at, pl.ds((stage - 1) * group, group)]

    def landed(buffer, slot, stage, start, n):
        at = span(start, n)
        return buffer.at[slot, at] if stage == 0 else buffer.at[slot, at, pl.ds((stage - 1) * group, group)]

    def send_x(b, stage, k):
        start, n = x_pieces[b, stage][k]
        slot = landing[b] + (2 if stage else 0)
        sem = x_places[b, stage]
        return remote(sums(stage, b, start, n), landed(rx, slot, stage, start, n), cx_s.at[sem, k], cx_r.at[sem, k], x_dev)

    def send_y(stage, k):
        start, n = y_pieces[stage][k]
        return remote(sums(stage, YN, start, n), landed(ry, 1 if stage else 0, stage, start, n), cy_s.at[stage, k], cy_r.at[stage, k], y_dev)

    late_o = remote(o_out, o_in, o_s, o_r, x_dev)

    def add_rows(part, b, start, n, got, col=0, n_col=half_w):
        at, cols = span(b * rows + start, n), pl.ds(col, n_col)
        acc[part, at, cols] = acc[part, at, cols] + got[:, cols]

    def finish(part, start, n, col=0, n_col=half_w):
        at, cols = span(start, n), pl.ds(col, n_col)
        first = acc[part, at, cols] + weighted(last, start, n, part, col, n_col)
        acc[part, at, cols] = first + weighted(n_own + last, start, n, part, col, n_col)

    before_last = await_second(last - 1)
    apply(before_last, XN, 0, rows)
    early = await_first(last)
    apply(early, XN, 0, rows)
    send_x(XN, 0, 0).start()
    apply(before_last, DG, 0, rows)
    apply(early, DG, 0, rows)
    late = await_second(last)
    pl.when(c == 1)(send_down)
    for k, (start, n) in enumerate(pieces):
        apply(late, DG, start, n)
        send_x(DG, 0, k).start()
    gate_up(late, XN * rows + kept, late_rows)
    o_out[...] = expert_rows(late, XN * rows + kept, late_rows, y)
    late_o.start()
    apply(late, XN, 0, kept)
    send_x(XN, 0, 1).start()
    for s in (before_last, early, late):
        for b in (YN, OWN):
            apply(s, b, 0, rows)

    def arrive_d(g, i):
        arrived_d(g, i).wait_recv()
        fwd_d(g, i).start()

    def round_two(i, carry, g=0):
        arrive_d(g, i)
        down(i, g)
        fwd_d(g, i).wait_recv()
        down(n_own + i, g)
        return carry

    def close_two(g, b):
        def step(k, carry):
            finish(oy, b * rows + k * (rows // 2), rows // 2, g * group, group)
            return carry

        lax.fori_loop(0, 2, step, 0)

    lax.fori_loop(0, n_own - 1, functools.partial(round_two, g=0), 0)
    arrive_d(0, last)
    fwd_d(0, last).wait_recv()

    def add_x(part, b, stage, k):
        start, n = x_pieces[b, stage][k]
        send_x(b, stage, k).wait_recv()
        slot = landing[b] + (2 if stage else 0)
        add_rows(part, YN if b == DG else OWN, start, n, rx.at[slot, span(start, n)], *columns(stage))

    def add_y(part, stage, k):
        start, n = y_pieces[stage][k]
        send_y(stage, k).wait_recv()
        add_rows(part, OWN, start, n, ry.at[1 if stage else 0, span(start, n)], *columns(stage))

    def columns(stage):
        return (0, half_w) if stage == 0 else ((stage - 1) * group, group)

    close_two(0, DG)
    send_x(DG, 1, 0).start()

    def others(b, carry):
        close_two(0, b)
        return carry

    lax.fori_loop(OWN, DG, others, 0)
    for k in range(n_first):
        add_x(y, DG, 0, k)
    send_y(0, 0).start()

    lax.fori_loop(0, n_own - 1, functools.partial(round_two, g=1), 0)
    arrive_d(1, last)
    fwd_d(1, last).wait_recv()
    close_two(1, DG)
    send_x(DG, 2, 0).start()
    send_x(XN, 1, 0).start()
    close_two(1, XN)
    for k in range(len(fine)):
        send_x(XN, 2, k).start()
    close_two(1, YN)
    add_x(oy, DG, 1, 0)
    send_y(1, 0).start()
    close_two(1, OWN)
    add_x(oy, DG, 2, 0)
    for k in range(len(fine)):
        send_y(2, k).start()
    add_x(y, XN, 0, 0)
    add_x(y, XN, 0, 1)
    late_o.wait_recv()
    at_late = span(kept, late_rows)
    acc[y, at_late, :] = acc[y, at_late, :] + scaled(gcol_x[at_late, :], late, o_in[...])
    add_y(oy, 0, 0)
    add_y(y, 1, 0)
    add_x(oy, XN, 1, 0)

    def result(k):
        start, n = fine[k]
        return pltpu.make_async_copy(tok.at[span(start, n)], out_hbm.at[span(start, n)], out_sem.at[k])

    for k, (start, n) in enumerate(fine):
        at = span(start, n)
        add_y(y, 2, k)
        add_x(oy, XN, 2, k)
        cut = n // 2 if n > tile else n
        for a in range(start, start + n, cut):
            rows_at = span(a, cut)
            for part in range(2):
                cols = pl.ds(part * half_w, half_w)
                tok[rows_at, cols] = (tok[rows_at, cols].astype(jnp.float32) + acc[part, rows_at, :]).astype(tok.dtype)
        result(k).start()

    def drain_w(i, carry):
        for m in range(3):
            partner_own(m, i).wait_send()
        for m in range(2):
            send_w(m, i).wait_send()
            partner_fwd(m, i).wait_send()
        for g in range(2):
            send_d(g, i).wait_send()
            fwd_d(g, i).wait_send()
        return carry

    lax.fori_loop(0, n_own, drain_w, 0)
    for (b, stage), some in x_pieces.items():
        for k in range(len(some)):
            send_x(b, stage, k).wait_send()
    for stage, some in enumerate(y_pieces):
        for k in range(len(some)):
            send_y(stage, k).wait_send()
    pl.when(c == 0)(tok_y.wait_send)
    for cp in (late_o, tok_x, tok_d, g_x, g_y, g_d):
        cp.wait_send()
    for k in range(len(fine)):
        result(k).wait()


def solution(mesh):
    ep_size = mesh.shape["ep"]
    row_spec = P(("rep", "ep", "fsdp"), None)

    def device_step(tokens, expert_idx, gates, w_gate, w_up, w_down):
        rows, top_k = expert_idx.shape
        n_local, half_w, ffn = w_gate.shape
        width = tokens.shape[1]
        n_own = n_local // 2
        num_experts = n_local * ep_size
        capacity = (2 * rows * top_k + num_experts - 1) // num_experts
        chunk, late_rows = 64, 160
        dma = pltpu.SemaphoreType.DMA
        hbm = pl.BlockSpec(memory_space=pl.ANY)
        return pl.pallas_call(
            functools.partial(moe_kernel, num_experts, capacity, chunk, late_rows),
            out_shape=pltpu.VMEM((rows, width), jnp.bfloat16),
            in_specs=[hbm] * 6,
            out_specs=hbm,
            scratch_shapes=[
                pltpu.VMEM((top_k, rows), jnp.int32),
                pltpu.VMEM((top_k, rows), jnp.float32),
                pltpu.VMEM((4 * rows, width), jnp.bfloat16),
                pltpu.VMEM((3, n_local, 2, half_w, ffn), jnp.bfloat16),
                pltpu.VMEM((2, 4 * rows, half_w), jnp.float32),
                pltpu.VMEM((n_local, 4 * rows, ffn), jnp.bfloat16),
                pltpu.VMEM((num_experts, rows), jnp.float32),
                pltpu.VMEM((4 * n_local, rows), jnp.float32),
                pltpu.VMEM((4 * rows, 128), jnp.float32),
                pltpu.VMEM((rows, 128), jnp.float32),
                pltpu.VMEM((4, rows, half_w), jnp.float32),
                pltpu.VMEM((2, rows, half_w), jnp.float32),
                pltpu.VMEM((late_rows, half_w), jnp.bfloat16),
                pltpu.VMEM((late_rows, half_w), jnp.bfloat16),
                pltpu.SemaphoreType.REGULAR,
                dma((2,)), dma((3,)), dma, dma((3,)), dma((3,)), dma((3,)), dma((3,)),
                dma((3, n_own)), dma((3, n_own)), dma((3, n_own)),
                dma((3, n_own)), dma((3, n_own)), dma((2, n_own)), dma((2, n_own)),
                dma((2, n_own)), dma((2, n_own)), dma((2, n_own)), dma((2, n_own)),
                dma((6, 4)), dma((6, 4)), dma((3, 3)), dma((3, 3)), dma, dma,
            ],
            compiler_params=pltpu.CompilerParams(collective_id=0, has_side_effects=True, vmem_limit_bytes=64_900_000),
        )(tokens, expert_idx.T, gates.T, w_gate, w_up, w_down)

    return jax.shard_map(device_step, mesh=mesh, in_specs=(row_spec, row_spec, row_spec, P("ep", "fsdp", None), P("ep", "fsdp", None), P("ep", None, "fsdp")), out_specs=row_spec, check_vma=False)
```

```python
import functools

import jax
import jax.numpy as jnp
from jax import lax
from jax.experimental import pallas as pl
from jax.experimental.pallas import tpu as pltpu
from jax.sharding import PartitionSpec as P

MESH = pl.DeviceIdType.MESH
OWN, XN, YN, DG = 0, 1, 2, 3


def moe_kernel(num_experts, capacity, chunk, late_rows, tokens_hbm, idx_hbm, gates_hbm, wg_hbm, wu_hbm, wd_hbm, out_hbm,
               idx_ref, gates_ref, tok, w, acc, hid, gt_send, gt_recv, gcol, gcol_x, rx, ry, o_out, o_in, go_sem,
               small_sem, out_sem, loc_tok_sem, tok_send, tok_recv, g_send, g_recv_sem, loc_sem, ys_sem, yr_sem,
               po_s, po_r, pf_s, pf_r, ds_sem, dr_sem, df_s, df_r, cx_s, cx_r, cy_s, cy_r, o_s, o_r):
    rows, width = out_hbm.shape
    n_local = wg_hbm.shape[0]
    n_own = n_local // 2
    half_w = width // 2
    group = half_w // 2
    n_chunk = rows // chunk
    ep = lax.axis_index("ep")
    y = lax.axis_index("fsdp")
    c = lax.rem(ep, 2)
    x = ep // 2
    oy = 1 - y
    x_dev = {"ep": lax.rem(ep + 2, 4), "fsdp": y}
    y_dev = {"ep": ep, "fsdp": oy}
    p_dev = {"ep": ep + 1 - 2 * c, "fsdp": y}
    w_hbm = (wg_hbm, wu_hbm, wd_hbm)

    def remote(src, dst, s, r, dev):
        return pltpu.make_async_remote_copy(src_ref=src, dst_ref=dst, send_sem=s, recv_sem=r, device_id=dev, device_id_type=MESH)

    def span(start, n):
        return pl.ds(pl.multiple_of(start, 16), n)

    def block(b):
        return tok.at[pl.ds(b * rows, rows)]

    idx_in = pltpu.make_async_copy(idx_hbm, idx_ref, small_sem.at[0])
    gates_in = pltpu.make_async_copy(gates_hbm, gates_ref, small_sem.at[1])
    idx_in.start()
    gates_in.start()
    barrier = pltpu.get_barrier_semaphore()
    for dev in (y_dev, x_dev, p_dev):
        pl.semaphore_signal(barrier, inc=1, device_id=dev, device_id_type=MESH)
    pl.semaphore_wait(barrier, 3)

    tok_y = remote(tokens_hbm, block(YN), tok_send.at[0], tok_recv.at[0], y_dev)
    tok_x = remote(tokens_hbm, block(XN), tok_send.at[1], tok_recv.at[1], x_dev)
    tok_d = remote(block(YN), block(DG), tok_send.at[2], tok_recv.at[2], x_dev)
    tok_l = pltpu.make_async_copy(tokens_hbm, block(OWN), loc_tok_sem)
    tok_x.start()
    tok_l.start()

    @pl.when(c == 1)
    def _():
        tok_y.start()

    row = lax.broadcasted_iota(jnp.int32, (num_experts, 1), 0)
    dest, slot = row // n_local, lax.rem(row, n_local)
    dx, dy = lax.rem(dest, 2), dest // 2
    ex = x + dx - 2 * x * dx
    ey = y + dy - 2 * y * dy
    sc = slot // n_own
    ec = c + sc - 2 * c * sc
    expert = (2 * ex + ec) * n_local + ey * n_own + lax.rem(slot, n_own)
    idx_in.wait()
    gates_in.wait()
    dense = jnp.zeros((num_experts, rows), jnp.float32)
    chosen = jnp.zeros((num_experts, rows), jnp.float32)
    for j in range(idx_ref.shape[0]):
        hit = idx_ref[j:j + 1, :] == expert
        dense = jnp.where(hit, gates_ref[j:j + 1, :], dense)
        chosen = jnp.where(hit, 1.0, chosen)
    before = lax.broadcasted_iota(jnp.int32, (rows, rows), 0) < lax.broadcasted_iota(jnp.int32, (rows, rows), 1)
    taken = jnp.dot(chosen.astype(jnp.bfloat16), before.astype(jnp.bfloat16), preferred_element_type=jnp.float32)
    dense = jnp.where(taken < float(capacity), dense, 0.0)
    gt_send[...] = dense
    g_x = remote(gt_send.at[pl.ds(XN * n_local, n_local)], gt_recv.at[pl.ds(0, n_local)], g_send.at[0], g_recv_sem.at[0], x_dev)
    g_y = remote(gt_send.at[pl.ds(YN * n_local, 2 * n_local)], gt_recv.at[pl.ds(n_local, 2 * n_local)], g_send.at[1], g_recv_sem.at[1], y_dev)
    g_d = remote(gt_recv.at[pl.ds(2 * n_local, n_local)], gt_recv.at[pl.ds(3 * n_local, n_local)], g_send.at[2], g_recv_sem.at[2], x_dev)


    g_x.start()

    def local_w(m, i):
        return pltpu.make_async_copy(w_hbm[m].at[y * n_own + i], w.at[m, i, y], loc_sem.at[m, i])

    def send_w(m, i):
        return remote(w_hbm[m].at[oy * n_own + i], w.at[m, i, y], ys_sem.at[m, i], yr_sem.at[m, i], y_dev)

    def arrived_w(m, i):
        return remote(w_hbm[m].at[oy * n_own + i], w.at[m, i, oy], ys_sem.at[m, i], yr_sem.at[m, i], y_dev)

    def partner_own(m, i):
        return remote(w_hbm[m].at[y * n_own + i], w.at[m, n_own + i, y], po_s.at[m, i], po_r.at[m, i], p_dev)

    def partner_fwd(m, i):
        return remote(w.at[m, i, oy], w.at[m, n_own + i, oy], pf_s.at[m, i], pf_r.at[m, i], p_dev)

    def down_half(slot, part, g):
        return w.at[2, slot, part, :, pl.ds(g * group, group)]

    def send_d(g, i):
        return remote(wd_hbm.at[oy * n_own + i, :, pl.ds(g * group, group)], down_half(i, y, g), ds_sem.at[g, i], dr_sem.at[g, i], y_dev)

    def arrived_d(g, i):
        return remote(wd_hbm.at[oy * n_own + i, :, pl.ds(g * group, group)], down_half(i, oy, g), ds_sem.at[g, i], dr_sem.at[g, i], y_dev)

    def fwd_d(g, i):
        return remote(down_half(i, oy, g), down_half(n_own + i, oy, g), df_s.at[g, i], df_r.at[g, i], p_dev)

    def send_gate_up():
        for i in range(n_own):
            for m in range(2):
                send_w(m, i).start()

    @pl.when(c == 1)
    def _():
        g_y.start()
        send_gate_up()

    def all_first(part):
        return remote(wd_hbm.at[pl.ds(oy * n_own, n_own), :, pl.ds(0, group)], w.at[2, pl.ds(0, n_own), part, :, pl.ds(0, group)],
                      ds_sem.at[0, 0], dr_sem.at[0, 0], y_dev)

    def send_down():
        all_first(y).start()
        for i in range(n_own):
            send_d(1, i).start()

    for i in range(n_own):
        for m in range(3):
            local_w(m, i).start()
            partner_own(m, i).start()

    def clear(k, carry):
        for part in range(2):
            acc[part, span(k * chunk, chunk), :] = jnp.zeros((chunk, half_w), jnp.float32)
        return carry

    lax.fori_loop(0, 4 * n_chunk, clear, 0)

    @pl.when(c == 1)
    def _():
        tok_y.wait_send()
        pl.semaphore_signal(go_sem, inc=1, device_id=p_dev, device_id_type=MESH)

    @pl.when(c == 0)
    def _():
        pl.semaphore_wait(go_sem, 1)
        tok_y.start()
        g_y.start()
        send_gate_up()
        send_down()

    def columns_of(g):
        return jnp.concatenate([g, jnp.zeros((128 - n_local, rows), jnp.float32)], axis=0).T

    def column_gates(b, g):
        gcol[pl.ds(b * rows, rows), :] = columns_of(g)

    column_gates(OWN, gt_send[0:n_local, :])
    gcol_x[...] = columns_of(gt_send[pl.ds(XN * n_local, n_local), :])
    tok_y.wait_recv()
    tok_d.start()
    g_y.wait_recv()
    g_d.start()
    for k, (b, cp) in enumerate(((XN, g_x), (YN, None), (None, None), (DG, g_d))):
        if cp is not None:
            cp.wait_recv()
        if b is not None:
            column_gates(b, gt_recv[k * n_local:(k + 1) * n_local, :])

    tok_l.wait()
    tok_x.wait_recv()
    tok_d.wait_recv()

    lane = lax.broadcasted_iota(jnp.int32, (1, 128), 1)

    def gate_up(s, start, n):
        at = span(start, n)
        r = tok[at, :]
        a = jnp.dot(r, w[0, s].reshape(width, w.shape[-1]), preferred_element_type=jnp.float32)
        u = jnp.dot(r, w[1, s].reshape(width, w.shape[-1]), preferred_element_type=jnp.float32)
        hid[s, at, :] = (a * jax.nn.sigmoid(a) * u).astype(jnp.bfloat16)

    def expert_rows(s, start, n, part, col=0, n_col=half_w):
        return jnp.dot(hid[s, span(start, n), :], w[2, s, part, :, pl.ds(col, n_col)], preferred_element_type=jnp.float32).astype(jnp.bfloat16)

    def scaled(gates, s, o):
        g = jnp.sum(jnp.where(lane == s, gates, 0.0), axis=1, keepdims=True)
        return jnp.where(g != 0.0, g * o.astype(jnp.float32), 0.0)

    def weighted(s, start, n, part, col=0, n_col=half_w):
        return scaled(gcol[span(start, n), :], s, expert_rows(s, start, n, part, col, n_col))

    def down(s, g):
        cols = pl.ds(g * group, group)
        step_rows = rows // 2

        def step(k, carry):
            at = span(k * step_rows, step_rows)
            acc[oy, at, cols] = acc[oy, at, cols] + weighted(s, k * step_rows, step_rows, oy, g * group, group)
            return carry

        lax.fori_loop(0, 8, step, 0)

    def arrive(m, i):
        arrived_w(m, i).wait_recv()
        partner_fwd(m, i).start()

    def await_own(i):
        for m in range(2):
            arrive(m, i)
        for m in range(3):
            local_w(m, i).wait()

    def await_partner(i):
        for m in range(3):
            partner_own(m, i).wait_recv()
        for m in range(2):
            partner_fwd(m, i).wait_recv()

    def await_first(i):
        pl.when(c == 0)(functools.partial(await_partner, i))
        pl.when(c == 1)(functools.partial(await_own, i))
        return i + n_own * (1 - c)

    def await_second(i):
        pl.when(c == 0)(functools.partial(await_own, i))
        pl.when(c == 1)(functools.partial(await_partner, i))
        return i + n_own * c

    def apply(s, b, start, n):
        size = n if n < rows // 2 else rows // 2 if n % (rows // 2) == 0 else n // 2

        def step(k, carry):
            first = b * rows + start + k * size
            at = span(first, size)
            gate_up(s, first, size)
            acc[y, at, :] = acc[y, at, :] + weighted(s, first, size, y)
            return carry

        lax.fori_loop(0, n // size, step, 0)

    def all_rows(s):
        def step(b, carry):
            apply(s, b, 0, rows)
            return carry

        lax.fori_loop(0, 4, step, 0)

    def round_one(i, carry):
        all_rows(await_first(i))
        all_rows(await_second(i))
        return carry

    last = n_own - 1
    lax.fori_loop(0, last - 1, round_one, 0)
    all_rows(await_first(last - 1))

    tile = 2 * chunk
    kept = rows - late_rows
    pieces = [(0, chunk), (chunk, chunk), (tile, tile), (2 * tile, rows - 2 * tile)]
    n_first = len(pieces)
    whole = [(0, rows)]
    fine = [(0, rows - tile), (rows - tile, tile - 32), (rows - 32, 32)]

    x_pieces = {(DG, 0): pieces, (XN, 0): [(kept, late_rows), (0, kept)], (DG, 1): whole, (DG, 2): whole, (XN, 1): whole, (XN, 2): fine}
    y_pieces = (whole, whole, fine)
    x_places = {kind: n for n, kind in enumerate(x_pieces)}
    landing = {DG: 0, XN: 1}

    def sums(stage, b, start, n):
        at = span(b * rows + start, n)
        return acc.at[y, at] if stage == 0 else acc.at[oy, at, pl.ds((stage - 1) * group, group)]

    def landed(buffer, slot, stage, start, n):
        at = span(start, n)
        return buffer.at[slot, at] if stage == 0 else buffer.at[slot, at, pl.ds((stage - 1) * group, group)]

    def send_x(b, stage, k):
        start, n = x_pieces[b, stage][k]
        slot = landing[b] + (2 if stage else 0)
        sem = x_places[b, stage]
        return remote(sums(stage, b, start, n), landed(rx, slot, stage, start, n), cx_s.at[sem, k], cx_r.at[sem, k], x_dev)

    def send_y(stage, k):
        start, n = y_pieces[stage][k]
        return remote(sums(stage, YN, start, n), landed(ry, 1 if stage else 0, stage, start, n), cy_s.at[stage, k], cy_r.at[stage, k], y_dev)

    late_o = remote(o_out, o_in, o_s, o_r, x_dev)

    def add_rows(part, b, start, n, got, col=0, n_col=half_w):
        at, cols = span(b * rows + start, n), pl.ds(col, n_col)
        acc[part, at, cols] = acc[part, at, cols] + got[:, cols]

    def finish(part, start, n, col=0, n_col=half_w):
        at, cols = span(start, n), pl.ds(col, n_col)
        first = acc[part, at, cols] + weighted(last, start, n, part, col, n_col)
        acc[part, at, cols] = first + weighted(n_own + last, start, n, part, col, n_col)

    before_last = await_second(last - 1)
    apply(before_last, XN, 0, rows)
    early = await_first(last)
    apply(early, XN, 0, rows)
    send_x(XN, 0, 0).start()
    apply(before_last, DG, 0, rows)
    apply(early, DG, 0, rows)
    late = await_second(last)
    pl.when(c == 1)(send_down)
    for k, (start, n) in enumerate(pieces):
        apply(late, DG, start, n)
        send_x(DG, 0, k).start()
    gate_up(late, XN * rows + kept, late_rows)
    o_out[...] = expert_rows(late, XN * rows + kept, late_rows, y)
    late_o.start()
    apply(late, XN, 0, kept)
    send_x(XN, 0, 1).start()
    for s in (before_last, early, late):
        for b in (YN, OWN):
            apply(s, b, 0, rows)

    def arrive_d(g, i):
        if g == 1:
            arrived_d(g, i).wait_recv()
            fwd_d(g, i).start()

    def round_two(i, carry, g=0):
        arrive_d(g, i)
        down(i, g)
        fwd_d(g, i).wait_recv()
        down(n_own + i, g)
        return carry

    def close_two(g, b):
        def step(k, carry):
            finish(oy, b * rows + k * (rows // 2), rows // 2, g * group, group)
            return carry

        lax.fori_loop(0, 2, step, 0)

    all_first(oy).wait_recv()
    for i in range(n_own):
        fwd_d(0, i).start()
    lax.fori_loop(0, n_own - 1, functools.partial(round_two, g=0), 0)
    arrive_d(0, last)
    fwd_d(0, last).wait_recv()

    def add_x(part, b, stage, k):
        start, n = x_pieces[b, stage][k]
        send_x(b, stage, k).wait_recv()
        slot = landing[b] + (2 if stage else 0)
        add_rows(part, YN if b == DG else OWN, start, n, rx.at[slot, span(start, n)], *columns(stage))

    def add_y(part, stage, k):
        start, n = y_pieces[stage][k]
        send_y(stage, k).wait_recv()
        add_rows(part, OWN, start, n, ry.at[1 if stage else 0, span(start, n)], *columns(stage))

    def columns(stage):
        return (0, half_w) if stage == 0 else ((stage - 1) * group, group)

    close_two(0, DG)
    send_x(DG, 1, 0).start()

    def others(b, carry):
        close_two(0, b)
        return carry

    lax.fori_loop(OWN, DG, others, 0)
    for k in range(n_first):
        add_x(y, DG, 0, k)
    send_y(0, 0).start()

    lax.fori_loop(0, n_own - 1, functools.partial(round_two, g=1), 0)
    arrive_d(1, last)
    fwd_d(1, last).wait_recv()
    close_two(1, DG)
    send_x(DG, 2, 0).start()
    send_x(XN, 1, 0).start()
    close_two(1, XN)
    for k in range(len(fine)):
        send_x(XN, 2, k).start()
    close_two(1, YN)
    add_x(oy, DG, 1, 0)
    send_y(1, 0).start()
    close_two(1, OWN)
    add_x(oy, DG, 2, 0)
    for k in range(len(fine)):
        send_y(2, k).start()
    add_x(y, XN, 0, 0)
    add_x(y, XN, 0, 1)
    late_o.wait_recv()
    at_late = span(kept, late_rows)
    acc[y, at_late, :] = acc[y, at_late, :] + scaled(gcol_x[at_late, :], late, o_in[...])
    add_y(oy, 0, 0)
    add_y(y, 1, 0)
    add_x(oy, XN, 1, 0)

    def result(k):
        start, n = fine[k]
        return pltpu.make_async_copy(tok.at[span(start, n)], out_hbm.at[span(start, n)], out_sem.at[k])

    for k, (start, n) in enumerate(fine):
        at = span(start, n)
        add_y(y, 2, k)
        add_x(oy, XN, 2, k)
        cut = n // 2 if n > tile else n
        for a in range(start, start + n, cut):
            rows_at = span(a, cut)
            for part in range(2):
                cols = pl.ds(part * half_w, half_w)
                tok[rows_at, cols] = (tok[rows_at, cols].astype(jnp.float32) + acc[part, rows_at, :]).astype(tok.dtype)
        result(k).start()

    def drain_w(i, carry):
        for m in range(3):
            partner_own(m, i).wait_send()
        for m in range(2):
            send_w(m, i).wait_send()
            partner_fwd(m, i).wait_send()
        send_d(1, i).wait_send()
        for g in range(2):
            fwd_d(g, i).wait_send()
        return carry

    lax.fori_loop(0, n_own, drain_w, 0)
    all_first(y).wait_send()
    for (b, stage), some in x_pieces.items():
        for k in range(len(some)):
            send_x(b, stage, k).wait_send()
    for stage, some in enumerate(y_pieces):
        for k in range(len(some)):
            send_y(stage, k).wait_send()
    pl.when(c == 0)(tok_y.wait_send)
    for cp in (late_o, tok_x, tok_d, g_x, g_y, g_d):
        cp.wait_send()
    for k in range(len(fine)):
        result(k).wait()


def solution(mesh):
    ep_size = mesh.shape["ep"]
    row_spec = P(("rep", "ep", "fsdp"), None)

    def device_step(tokens, expert_idx, gates, w_gate, w_up, w_down):
        rows, top_k = expert_idx.shape
        n_local, half_w, ffn = w_gate.shape
        width = tokens.shape[1]
        n_own = n_local // 2
        num_experts = n_local * ep_size
        capacity = (2 * rows * top_k + num_experts - 1) // num_experts
        chunk, late_rows = 64, 160
        dma = pltpu.SemaphoreType.DMA
        hbm = pl.BlockSpec(memory_space=pl.ANY)
        return pl.pallas_call(
            functools.partial(moe_kernel, num_experts, capacity, chunk, late_rows),
            out_shape=pltpu.VMEM((rows, width), jnp.bfloat16),
            in_specs=[hbm] * 6,
            out_specs=hbm,
            scratch_shapes=[
                pltpu.VMEM((top_k, rows), jnp.int32),
                pltpu.VMEM((top_k, rows), jnp.float32),
                pltpu.VMEM((4 * rows, width), jnp.bfloat16),
                pltpu.VMEM((3, n_local, 2, half_w, ffn), jnp.bfloat16),
                pltpu.VMEM((2, 4 * rows, half_w), jnp.float32),
                pltpu.VMEM((n_local, 4 * rows, ffn), jnp.bfloat16),
                pltpu.VMEM((num_experts, rows), jnp.float32),
                pltpu.VMEM((4 * n_local, rows), jnp.float32),
                pltpu.VMEM((4 * rows, 128), jnp.float32),
                pltpu.VMEM((rows, 128), jnp.float32),
                pltpu.VMEM((4, rows, half_w), jnp.float32),
                pltpu.VMEM((2, rows, half_w), jnp.float32),
                pltpu.VMEM((late_rows, half_w), jnp.bfloat16),
                pltpu.VMEM((late_rows, half_w), jnp.bfloat16),
                pltpu.SemaphoreType.REGULAR,
                dma((2,)), dma((3,)), dma, dma((3,)), dma((3,)), dma((3,)), dma((3,)),
                dma((3, n_own)), dma((3, n_own)), dma((3, n_own)),
                dma((3, n_own)), dma((3, n_own)), dma((2, n_own)), dma((2, n_own)),
                dma((2, n_own)), dma((2, n_own)), dma((2, n_own)), dma((2, n_own)),
                dma((6, 4)), dma((6, 4)), dma((3, 3)), dma((3, 3)), dma, dma,
            ],
            compiler_params=pltpu.CompilerParams(collective_id=0, has_side_effects=True, vmem_limit_bytes=64_900_000),
        )(tokens, expert_idx.T, gates.T, w_gate, w_up, w_down)

    return jax.shard_map(device_step, mesh=mesh, in_specs=(row_spec, row_spec, row_spec, P("ep", "fsdp", None), P("ep", "fsdp", None), P("ep", None, "fsdp")), out_specs=row_spec, check_vma=False)
```
